8 devices in a mesh: dp: 1 (over z), etp: 2 (over y), ep: 4 (over x, core).
Axes of the slice: x: 2, y: 2, z: 1, core: 2. Of those that a mesh axis runs over, the one named last changes fastest.
Arguments:
- hidden: bfloat16 [512, 2048], P(('dp', 'ep'))
- expert_ids: int32 [512, 2], P(('dp', 'ep'))
- gate_wts: float32 [512, 2], P(('dp', 'ep'))
- slot_pos: int32 [512, 2], P(('dp', 'ep'))
- w_gate: bfloat16 [8, 2048, 5632], P('ep', None, 'etp')
- w_up: bfloat16 [8, 2048, 5632], P('ep', None, 'etp')
- w_down: bfloat16 [8, 5632, 2048], P('ep', 'etp')
Outputs:
- output: bfloat16 [512, 2048], P(('dp', 'ep'))
All inputs are finite; a program needn't handle non-finite values.
Results may differ from the reference program's by a relative error of at most 0.0012.
Values are sent between devices in bfloat16 or wider.
A program may use at most 1 GiB of HBM per device.

```python
import jax
import jax.numpy as jnp
from jax import lax

D_MODEL = 2048
D_FF = 5632
EXPERTS = 8
TOP_K = 2
TOK_DEV = 128
GROUP = 4
LOCAL_CAP = 40

TOKENS = TOK_DEV * GROUP
CAPACITY = LOCAL_CAP * GROUP


def rank_in_expert(flat_ids, priority):
    n_choices = flat_ids.shape[0]
    sort_order = jnp.argsort(flat_ids * n_choices + priority)
    sorted_ids = flat_ids[sort_order]
    counts = jnp.bincount(flat_ids, length=EXPERTS)
    starts = jnp.cumsum(counts) - counts
    sorted_rank = jnp.arange(n_choices) - starts[sorted_ids]
    return jnp.zeros((n_choices,), jnp.int32).at[sort_order].set(sorted_rank.astype(jnp.int32))


def draw_routing(route_key):
    key_hot, key_rows, key_bias, key_score, key_prio = jax.random.split(route_key, 5)
    hot_expert = jax.random.randint(key_hot, (GROUP,), 0, EXPERTS)
    row_perm = jax.vmap(lambda sub_key: jax.random.permutation(sub_key, TOK_DEV))(jax.random.split(key_rows, GROUP))
    forced = row_perm < LOCAL_CAP
    expert_bias = jax.random.randint(key_bias, (EXPERTS,), 0, 2 ** 19)
    scores = jax.random.randint(key_score, (GROUP, TOK_DEV, EXPERTS), 0, 2 ** 20) + expert_bias
    expert_range = jnp.arange(EXPERTS)
    is_hot = forced[:, :, None] & (expert_range[None, None, :] == hot_expert[:, None, None])
    scores = jnp.where(is_hot, 2 ** 21, scores)
    top_scores, expert_ids = lax.top_k(scores * EXPERTS + expert_range, TOP_K)
    priority = jax.vmap(lambda sub_key: jax.random.permutation(sub_key, TOK_DEV * TOP_K))(jax.random.split(key_prio, GROUP))
    local_rank = jax.vmap(rank_in_expert)(expert_ids.reshape(GROUP, TOK_DEV * TOP_K), priority)
    block_base = (jnp.arange(GROUP) * LOCAL_CAP)[:, None]
    slot_pos = jnp.where(local_rank < LOCAL_CAP, block_base + local_rank, -1)
    return expert_ids.reshape(TOKENS, TOP_K).astype(jnp.int32), slot_pos.reshape(TOKENS, TOP_K).astype(jnp.int32)


def setup_inputs(seed: int = 0, part: int = 0) -> dict:
    base_key = jax.random.key(seed)
    part_key = jax.random.fold_in(base_key, part)
    key_hidden, key_route, key_gate = jax.random.split(part_key, 3)
    key_w_gate, key_w_up, key_w_down = jax.random.split(jax.random.key(seed + 1), 3)
    hidden = jax.random.normal(key_hidden, (TOKENS, D_MODEL), jnp.float32).astype(jnp.bfloat16)
    expert_ids, slot_pos = draw_routing(key_route)
    logits = jax.random.normal(key_gate, (TOKENS, TOP_K), jnp.float32)
    gate_wts = jax.nn.softmax(logits, axis=-1)
    w_gate = (jax.random.normal(key_w_gate, (EXPERTS, D_MODEL, D_FF), jnp.float32) * D_MODEL ** -0.5).astype(jnp.bfloat16)
    w_up = (jax.random.normal(key_w_up, (EXPERTS, D_MODEL, D_FF), jnp.float32) * D_MODEL ** -0.5).astype(jnp.bfloat16)
    w_down = (jax.random.normal(key_w_down, (EXPERTS, D_FF, D_MODEL), jnp.float32) * D_FF ** -0.5).astype(jnp.bfloat16)
    return dict(hidden=hidden, expert_ids=expert_ids, gate_wts=gate_wts, slot_pos=slot_pos, w_gate=w_gate, w_up=w_up, w_down=w_down)


def reference(hidden, expert_ids, gate_wts, slot_pos, w_gate, w_up, w_down):
    flat_pos = slot_pos.reshape(-1)
    slot_index = jnp.where(flat_pos >= 0, expert_ids.reshape(-1) * CAPACITY + flat_pos, EXPERTS * CAPACITY)
    token_index = jnp.broadcast_to(jnp.arange(TOKENS, dtype=jnp.int32)[:, None], (TOKENS, TOP_K)).reshape(-1)
    slot_token = jnp.full((EXPERTS * CAPACITY,), TOKENS, jnp.int32).at[slot_index].set(token_index, mode='drop')
    slot_gate = jnp.zeros((EXPERTS * CAPACITY,), jnp.float32).at[slot_index].set(gate_wts.reshape(-1), mode='drop')

    def expert_step(running, operands):
        tok_ids, gate_col, gate_mat, up_mat, down_mat = operands
        buffer = jnp.take(hidden, tok_ids, axis=0, mode='fill', fill_value=0)
        h_gate = jnp.dot(buffer, gate_mat, preferred_element_type=jnp.float32)
        h_up = jnp.dot(buffer, up_mat, preferred_element_type=jnp.float32)
        hidden_act = (jax.nn.silu(h_gate) * h_up).astype(jnp.bfloat16)
        expert_out = jnp.dot(hidden_act, down_mat, preferred_element_type=jnp.float32)
        running = running + jax.ops.segment_sum(expert_out * gate_col[:, None], tok_ids, num_segments=TOKENS)
        return running, None

    start_sum = jnp.zeros((TOKENS, D_MODEL), jnp.float32)
    total_out, unused = lax.scan(expert_step, start_sum, (slot_token.reshape(EXPERTS, CAPACITY), slot_gate.reshape(EXPERTS, CAPACITY), w_gate, w_up, w_down))
    return total_out.astype(jnp.bfloat16)
```

```python
import functools
import jax
import jax.numpy as jnp
from jax import lax
from jax.sharding import PartitionSpec as P
from jax.experimental import pallas as pl
from jax.experimental.pallas import tpu as pltpu

MESH = pl.DeviceIdType.MESH
F32, BF16 = jnp.float32, jnp.bfloat16
N_Q = 4
N_U = 4
GU_SLOTS = 3
WD_SLOTS = 3
Y_FIRST = (0,)


def moe_kernel(rows, d_model, d_ff, cap_local,
               hid_hbm, ids_ref, gates_ref, pos_ref, wg_hbm, wu_hbm, wd_hbm, out_hbm,
               tok, route, onehot, comb, gate_col, xs, acc, act, wgu, wdn,
               w_own, w_send, w_recv, f1_keep, f1_send, f1_recv, f2_send, f2_recv, fin, outbuf,
               hid_sem, gu_sem, wd_sem, out_sem,
               rt_s, rt_r, s1_s, s1_r, xd_s, xd_r, yd_s, yd_r, c3_s, c3_r, c4_s, c4_r,
               dw_s, dw_r, f1_s, f1_r, f2_s, f2_r, fo_s, fo_r):
    cap = 4 * cap_local
    qw = d_model // N_Q
    hw = qw // 2
    uw = d_model // (2 * N_U)
    nh = d_ff // 2
    ep = lax.axis_index("ep")
    y = lax.axis_index("etp")
    c = lax.rem(ep, 2)
    x = ep // 2
    ox, oy, oc = 1 - x, 1 - y, 1 - c
    dev_c = {"ep": 2 * x + oc}
    dev_x = {"ep": 2 * ox + c}
    dev_xc = {"ep": 2 * ox + oc}
    dev_y = {"etp": oy}
    dev_yc = {"etp": oy, "ep": 2 * x + oc}
    dev_fin = {"etp": oy, "ep": 2 * x + y}

    def remote(src, dst, s, r, dev):
        return pltpu.make_async_remote_copy(src_ref=src, dst_ref=dst, send_sem=s, recv_sem=r,
                                            device_id=dev, device_id_type=MESH)

    hid_copy = pltpu.make_async_copy(hid_hbm, tok.at[pl.ds(ep * rows, rows)], hid_sem)
    hid_copy.start()

    def gu_copy(q, e, m):
        slot = (q % GU_SLOTS) * 2 + e
        src = (wg_hbm, wu_hbm)[m]
        return pltpu.make_async_copy(src.at[e, pl.ds(q * qw, qw)], wgu.at[slot, m], gu_sem.at[slot, m])

    def wd_copy(t, e):
        is_peer, u = unit_of(t)
        col = (jnp.where(is_peer, oc, c) * N_U + u) * uw
        slot = lax.rem(t, WD_SLOTS)
        return pltpu.make_async_copy(wd_hbm.at[e, :, pl.ds(pl.multiple_of(col, uw), uw)],
                                     wdn.at[slot, e], wd_sem.at[slot, e])

    def unit_of(t):
        is_peer = (t == 0) | ((lax.rem(t, 2) == 1) & (t < 2 * N_U - 1))
        return is_peer, jnp.where(is_peer, (t + 1) // 2, (t - 1) // 2)

    for q in range(GU_SLOTS):
        for e in range(2):
            for m in range(2):
                gu_copy(q, e, m).start()

    lane = lax.broadcasted_iota(jnp.int32, (rows, 128), 1)
    code = jnp.where(pos_ref[...] >= 0, ids_ref[...] * cap + pos_ref[...], -1).astype(F32)
    gts = gates_ref[...]
    cols = jnp.where(lane == 0, code[:, 0:1], jnp.where(lane == 1, code[:, 1:2],
                     jnp.where(lane == 2, gts[:, 0:1], gts[:, 1:2])))
    route[pl.ds(ep, 1)] = cols.T[0:8][None]

    barrier = pltpu.get_barrier_semaphore()
    for dev in (dev_c, dev_x, dev_xc, dev_y, dev_yc):
        pl.semaphore_signal(barrier, inc=1, device_id=dev, device_id_type=MESH)
    for t in range(WD_SLOTS):
        for e in range(2):
            wd_copy(jnp.int32(t), e).start()
    pl.semaphore_wait(barrier, 5)

    own = pl.ds(pl.multiple_of(ep * rows, rows), rows)
    of_c = pl.ds(pl.multiple_of((2 * x + oc) * rows, rows), rows)
    of_x = pl.ds(pl.multiple_of((2 * ox + c) * rows, rows), rows)
    of_xc = pl.ds(pl.multiple_of((2 * ox + oc) * rows, rows), rows)

    def piece(blk, q, half):
        start = q * qw if half is None else q * qw + half * hw
        return tok.at[blk, pl.ds(pl.multiple_of(start, 128), qw if half is None else hw)]

    def route_copy(i, dev, blk):
        return remote(route.at[blk], route.at[blk], rt_s.at[i], rt_r.at[i], dev)

    def s1(q, blk):
        return remote(piece(blk, q, None), piece(blk, q, None), s1_s.at[q], s1_r.at[q], dev_c)

    def s2(q, blk):
        return remote(piece(blk, q, y), piece(blk, q, y), xd_s.at[q], xd_r.at[q], dev_x)

    def s3y(q, half):
        return remote(piece(of_x, q, half), piece(of_x, q, half), yd_s.at[q], yd_r.at[q], dev_y)

    def s3c(q, blk):
        return remote(piece(blk, q, y), piece(blk, q, y), c3_s.at[q], c3_r.at[q], dev_c)

    def s4(q, blk):
        return remote(piece(blk, q, oy), piece(blk, q, oy), c4_s.at[q], c4_r.at[q], dev_c)

    for i, dev in enumerate((dev_c, dev_x, dev_xc)):
        route_copy(i, dev, ep).start()
    hid_copy.wait()
    for q in range(N_Q):
        s2(q, own).start()
    for q in range(N_Q):
        s1(q, own).start()

    @pl.loop(0, 4)
    def _(i):
        acc[i // 2, lax.rem(i, 2)] = jnp.zeros((cap, d_ff), F32)

    for i, blk in enumerate((2 * x + oc, 2 * ox + c, 2 * ox + oc)):
        route_copy(i, (dev_c, dev_x, dev_xc)[i], blk).wait_recv()

    def route_row(j):
        return jnp.concatenate([route[b, j:j + 1, :] for b in range(4)], axis=1)

    row_code = (route_row(0), route_row(1))
    row_gate = (route_row(2), route_row(3))
    for e in range(2):
        slot = (lax.broadcasted_iota(jnp.int32, (cap, 4 * rows), 0) + (2 * ep + e) * cap).astype(F32)
        hit0, hit1 = row_code[0] == slot, row_code[1] == slot
        onehot[e] = jnp.where(hit0 | hit1, 1.0, 0.0).astype(BF16)
        g = jnp.where(hit0, row_gate[0], 0.0) + jnp.where(hit1, row_gate[1], 0.0)
        gate_col[e] = jnp.sum(g, axis=1, keepdims=True)
    k = lax.broadcasted_iota(jnp.int32, (rows, 4 * cap_local), 1)
    part = jnp.where(k >= 2 * cap_local, 1, 0)
    k = k - part * (2 * cap_local)
    sub = jnp.where(k >= cap_local, 1, 0)
    k = k - sub * cap_local
    dev_of = jnp.where(part == 0, ep, 2 * x + oc)
    for b in range(4):
        slot = ((2 * dev_of + sub) * cap + b * cap_local + k).astype(F32)
        back = jnp.concatenate([route[b]] * 16, axis=0).T
        hit = (back[:, 0:1] == slot) | (back[:, 1:2] == slot)
        one = jnp.where(hit, 1.0, 0.0).astype(BF16)
        comb[b] = jnp.concatenate([one, one, one], axis=1)

    def relay_x(q):
        s2(q, of_x).wait_recv()
        s3y(q, y).start()
        s3c(q, of_x).start()

    def relay_y(q):
        s3y(q, oy).wait_recv()
        s4(q, of_x).start()

    relay_x(0)
    relay_x(1)
    relay_y(0)
    relay_x(2)
    between = {(0, 1): [(relay_y, 1)], (0, 2): [(relay_x, 3)], (0, 3): [(relay_y, 2)], (1, 1): [(relay_y, 3)]}

    for q in range(N_Q):
        s1(q, of_c).wait_recv()
        s3c(q, of_xc).wait_recv()
        s4(q, of_xc).wait_recv()
        for e in range(2):
            rows_q = jnp.dot(onehot[e], tok[:, q * qw:(q + 1) * qw], preferred_element_type=F32)
            xs[e] = rows_q.astype(BF16)

        @pl.loop(0, 4)
        def _(i, q=q):
            e, half = i // 2, lax.rem(i, 2)
            for j in (1, 2, 3):
                if (q, j) in between:
                    @pl.when(i == j)
                    def _(acts=between[(q, j)]):
                        for fn, arg in acts:
                            fn(arg)

            @pl.when(half == 0)
            def _():
                for m in range(2):
                    gu_copy(q, e, m).wait()

            span = pl.ds(pl.multiple_of(half * nh, 128), nh)
            slot = (q % GU_SLOTS) * 2 + e
            for m in range(2):
                acc[e, m, :, span] += jnp.dot(xs[e], wgu[slot, m, :, span], preferred_element_type=F32)
            if q + GU_SLOTS < N_Q:
                @pl.when(half == 1)
                def _():
                    for m in range(2):
                        gu_copy(q + GU_SLOTS, e, m).start()

    @pl.loop(0, 2 * 11)
    def _(i):
        e = i // 11
        span = pl.ds(pl.multiple_of(lax.rem(i, 11) * (d_ff // 11), 128), d_ff // 11)
        g = acc[e, 0, :, span]
        act[e, :, span] = (jax.nn.silu(g) * acc[e, 1, :, span]).astype(BF16)

    def dw(u):
        return remote(w_send.at[u], w_recv.at[u], dw_s.at[u], dw_r.at[u], dev_c)

    def first_dev(u):
        return dev_y if u in Y_FIRST else dev_x

    def second_dev(u):
        return dev_x if u in Y_FIRST else dev_y

    def f1(u):
        return remote(f1_send.at[u], f1_recv.at[u], f1_s.at[u], f1_r.at[u], first_dev(u))

    def f2(u):
        return remote(f2_send.at[u], f2_recv.at[u], f2_s.at[u], f2_r.at[u], second_dev(u))

    @pl.loop(0, 2 * N_U)
    def _(t):
        is_peer, u = unit_of(t)
        slot = lax.rem(t, WD_SLOTS)
        for e in range(2):
            wd_copy(t, e).wait()
        outs = [jnp.dot(act[e], wdn[slot, e], preferred_element_type=F32) * gate_col[e] for e in range(2)]

        @pl.when(is_peer)
        def _():
            for e in range(2):
                for b in range(4):
                    w_send[u, b, e * cap_local:(e + 1) * cap_local] = outs[e][b * cap_local:(b + 1) * cap_local]

        @pl.when(jnp.logical_not(is_peer))
        def _():
            for e in range(2):
                for b in range(4):
                    w_own[b, e * cap_local:(e + 1) * cap_local] = outs[e][b * cap_local:(b + 1) * cap_local]

        @pl.when(t + WD_SLOTS < 2 * N_U)
        def _():
            for e in range(2):
                wd_copy(t + WD_SLOTS, e).start()

        @pl.when(is_peer)
        def _():
            dw(u).start()

        @pl.when(jnp.logical_not(is_peer))
        def _():
            dw(u).wait_recv()
            y_first = functools.reduce(jnp.logical_or, [u == v for v in Y_FIRST], False)
            keep1 = jnp.where(y_first, 2 * ox + y, 2 * x + oy)
            send0 = jnp.where(y_first, 2 * x + oy, 2 * ox + y)
            for dst, pos, b in ((f1_send, 0, send0), (f1_send, 1, 2 * ox + oy),
                                (f1_keep, 0, 2 * x + y), (f1_keep, 1, keep1)):
                s = jnp.concatenate([w_own[b], w_recv[u, b]], axis=0)
                hi = s.astype(BF16)
                rest = s - hi.astype(F32)
                mid = rest.astype(BF16)
                lo = (rest - mid.astype(F32)).astype(BF16)
                parts = jnp.concatenate([hi, mid, lo], axis=0)
                dst[u, pos] = jnp.dot(comb[b], parts, preferred_element_type=F32)
            for v in range(N_U):
                @pl.when(u == v)
                def _(v=v):
                    f1(v).start()

    def out_cols(core, u):
        return pl.ds(pl.multiple_of((core * N_U + u) * uw, 128), uw)

    def to_other(u):
        return remote(fin.at[u], outbuf.at[:, out_cols(c, u)], fo_s.at[u, 0], fo_r.at[u, c], dev_fin)

    def to_core(u):
        return remote(fin.at[u], outbuf.at[:, out_cols(c, u)], fo_s.at[u, 1], fo_r.at[u, c], dev_c)

    def stage2(u):
        f1(u).wait_recv()
        f2_send[u] = f1_keep[u, 1] + f1_recv[u, 1]
        f2(u).start()
        f1_keep[u, 0] = f1_keep[u, 0] + f1_recv[u, 0]

    def stage3(u):
        f2(u).wait_recv()
        fin[u] = (f1_keep[u, 0] + f2_recv[u]).astype(BF16)
        to_other(u).start()

        @pl.when(c == y)
        def _():
            outbuf[:, out_cols(c, u)] = fin[u]

        @pl.when(c != y)
        def _():
            to_core(u).start()

    for u in range(N_U):
        stage2(u)
        if u >= 1:
            stage3(u - 1)
    stage3(N_U - 1)

    def incoming(u, core):
        return remote(fin.at[u], outbuf.at[:, out_cols(core, u)], fo_s.at[u, 0], fo_r.at[u, core], dev_fin)

    for u in range(N_U):
        incoming(u, oc).wait_recv()

        @pl.when(c != y)
        def _(u=u):
            incoming(u, c).wait_recv()

    out_copy = pltpu.make_async_copy(outbuf, out_hbm, out_sem)
    out_copy.start()

    for i, dev in enumerate((dev_c, dev_x, dev_xc)):
        route_copy(i, dev, ep).wait_send()
    for q in range(N_Q):
        s1(q, own).wait_send()
        s2(q, own).wait_send()
        s3y(q, y).wait_send()
        s3c(q, of_x).wait_send()
        s4(q, of_x).wait_send()
    for u in range(N_U):
        dw(u).wait_send()
        f1(u).wait_send()
        f2(u).wait_send()
        to_other(u).wait_send()

        @pl.when(c != y)
        def _(u=u):
            to_core(u).wait_send()
    out_copy.wait()


def solution(mesh):
    group = mesh.shape['ep']
    row_spec = P(('dp', 'ep'), None)
    col_spec = P('ep', None, 'etp')
    in_specs = (row_spec, row_spec, row_spec, row_spec, col_spec, col_spec, P('ep', 'etp', None))

    def device_step(hidden, expert_ids, gate_wts, slot_pos, w_gate, w_up, w_down):
        rows, d_model = hidden.shape
        top_k = expert_ids.shape[1]
        local_experts = w_gate.shape[0]
        experts = local_experts * group
        cap_local = ((5 * top_k * rows) // (4 * experts) + 7) // 8 * 8
        cap = group * cap_local
        d_ff = w_gate.shape[2]
        qw = d_model // N_Q
        uw = d_model // (2 * N_U)
        any_spec = pl.BlockSpec(memory_space=pl.ANY)
        vmem_spec = pl.BlockSpec(memory_space=pltpu.VMEM)
        dma = pltpu.SemaphoreType.DMA
        scratch = [
            pltpu.VMEM((group * rows, d_model), BF16),
            pltpu.VMEM((group, 8, 128), F32),
            pltpu.VMEM((2, cap, group * rows), BF16),
            pltpu.VMEM((group, rows, 12 * cap_local), BF16),
            pltpu.VMEM((2, cap, 1), F32),
            pltpu.VMEM((2, cap, qw), BF16),
            pltpu.VMEM((2, 2, cap, d_ff), F32),
            pltpu.VMEM((2, cap, d_ff), BF16),
            pltpu.VMEM((2 * GU_SLOTS, 2, qw, d_ff), BF16),
            pltpu.VMEM((WD_SLOTS, 2, d_ff, uw), BF16),
            pltpu.VMEM((4, 2 * cap_local, uw), F32),
            pltpu.VMEM((N_U, 4, 2 * cap_local, uw), F32),
            pltpu.VMEM((N_U, 4, 2 * cap_local, uw), F32),
            pltpu.VMEM((N_U, 2, rows, uw), F32),
            pltpu.VMEM((N_U, 2, rows, uw), F32),
            pltpu.VMEM((N_U, 2, rows, uw), F32),
            pltpu.VMEM((N_U, rows, uw), F32),
            pltpu.VMEM((N_U, rows, uw), F32),
            pltpu.VMEM((N_U, rows, uw), BF16),
            pltpu.VMEM((rows, d_model), BF16),
            dma, dma((2 * GU_SLOTS, 2)), dma((WD_SLOTS, 2)), dma,
            dma((3,)), dma((3,)),
        ] + [dma((N_Q,))] * 10 + [dma((N_U,))] * 6 + [dma((N_U, 2)), dma((N_U, 2))]
        return pl.pallas_call(
            functools.partial(moe_kernel, rows, d_model, d_ff, cap_local),
            out_shape=jax.ShapeDtypeStruct((rows, d_model), BF16),
            in_specs=[any_spec, vmem_spec, vmem_spec, vmem_spec, any_spec, any_spec, any_spec],
            out_specs=any_spec,
            scratch_shapes=scratch,
            compiler_params=pltpu.CompilerParams(collective_id=0, has_side_effects=True,
                                                 vmem_limit_bytes=67_043_328),
        )(hidden, expert_ids, gate_wts, slot_pos, w_gate, w_up, w_down)

    return jax.shard_map(device_step, mesh=mesh, in_specs=in_specs, out_specs=row_spec, check_vma=False)
```

```python
import functools
import jax
import jax.numpy as jnp
from jax import lax
from jax.sharding import PartitionSpec as P
from jax.experimental import pallas as pl
from jax.experimental.pallas import tpu as pltpu

MESH = pl.DeviceIdType.MESH
F32, BF16 = jnp.float32, jnp.bfloat16
N_W = 4
GU_SLOTS = 3
WD_SLOTS = 3
N_U = 8
NB = 512
PIECE = 256
CHUNKS = ((0, 1, True), (1, 1, True), (2, 2, False), (4, 2, False), (6, 2, False))
Y_FIRST = (1, 3, 7)
ORDER = (
    "D0", "D1", "D2", "C0", "S0", "C1", "S1", "H0", "H1", "D3", "C2", "D4",
    "D5", "S2", "C3", "S3", "H2", "D6", "D7", "H3", "C5", "A0", "S5", "C4",
    "C6", "C7", "S7", "S6", "S4", "H5", "H7", "A2", "A3", "H6", "A1", "A6",
    "H4", "A5", "A4", "B2", "B6", "A7", "B0", "B5", "B1", "B4", "B3", "B7",
)


def moe_kernel(rows, d_model, d_ff, cap_local,
               hid_hbm, ids_ref, gates_ref, pos_ref, wg_hbm, wu_hbm, wd_hbm, out_hbm,
               tok, route, onehot, comb, gate_col, xs, acc, act, wgu, wdn,
               w_all, w_recv, f1_keep, f1_send, f1_recv, f2_send, f2_recv, fin,
               hid_sem, gu_sem, wd_sem,
               rt_s, rt_r, s1_s, s1_r, xd_s, xd_r, yd_s, yd_r, c3_s, c3_r, c4_s, c4_r,
               dw_s, dw_r, f1_s, f1_r, f2_s, f2_r, fo_s, fo_r):
    cap = 4 * cap_local
    kw = d_model // N_W
    uw = d_model // N_U
    hu = uw // 2
    ep = lax.axis_index("ep")
    y = lax.axis_index("etp")
    c = lax.rem(ep, 2)
    x = ep // 2
    ox, oy, oc = 1 - x, 1 - y, 1 - c
    dev_c = {"ep": 2 * x + oc}
    dev_x = {"ep": 2 * ox + c}
    dev_xc = {"ep": 2 * ox + oc}
    dev_y = {"etp": oy}
    dev_yc = {"etp": oy, "ep": 2 * x + oc}
    dev_fin = {"etp": oy, "ep": 2 * x + y}
    always = ep >= 0

    def remote(src, dst, s, r, dev):
        return pltpu.make_async_remote_copy(src_ref=src, dst_ref=dst, send_sem=s, recv_sem=r,
                                            device_id=dev, device_id_type=MESH)

    def block(b):
        return pl.ds(pl.multiple_of(b * rows, rows), rows)

    own, of_c, of_x, of_xc = block(ep), block(2 * x + oc), block(2 * ox + c), block(2 * ox + oc)

    def hid_copy(i):
        return pltpu.make_async_copy(hid_hbm.at[:, i * PIECE:(i + 1) * PIECE], tok.at[i, own], hid_sem.at[i])

    def gu_copy(w, e, m):
        slot = (w % GU_SLOTS) * 2 + e
        src = (wg_hbm, wu_hbm)[m]
        return pltpu.make_async_copy(src.at[e, pl.ds(w * kw, kw)], wgu.at[slot, m], gu_sem.at[slot, m])

    def wd_copy(u, e):
        slot = u % WD_SLOTS
        return pltpu.make_async_copy(wd_hbm.at[e, :, pl.ds(u * uw, uw)], wdn.at[slot, e], wd_sem.at[slot, e])

    for i in range(d_model // PIECE):
        hid_copy(i).start()

    code = jnp.where(pos_ref[...] >= 0, ids_ref[...] * cap + pos_ref[...], -1).astype(F32)
    route[ep] = jnp.concatenate([code, gates_ref[...], jnp.zeros((4, rows), F32)], axis=0)

    barrier = pltpu.get_barrier_semaphore()
    for dev in (dev_c, dev_x, dev_xc, dev_y, dev_yc):
        pl.semaphore_signal(barrier, inc=1, device_id=dev, device_id_type=MESH)
    with jax.named_scope("hid_wait"):
        for i in range(d_model // PIECE):
            hid_copy(i).wait()
    for w in range(GU_SLOTS):
        for e in range(2):
            for m in range(2):
                gu_copy(w, e, m).start(priority=1)
    for u in range(WD_SLOTS):
        for e in range(2):
            wd_copy(u, e).start(priority=1)
    with jax.named_scope("barrier"):
        pl.semaphore_wait(barrier, 5)

    def pieces(k, blk, half):
        first, n, direct = CHUNKS[k]
        return tok.at[pl.ds(first, n), blk] if half is None or direct else tok.at[first + half, blk]

    def route_copy(i, dev, b):
        return remote(route.at[b], route.at[b], rt_s.at[i], rt_r.at[i], dev)

    def to_core_own(k, blk):
        return remote(pieces(k, blk, None), pieces(k, blk, None), s1_s.at[k], s1_r.at[k], dev_c)

    def over_x(k, blk):
        return remote(pieces(k, blk, y), pieces(k, blk, y), xd_s.at[k], xd_r.at[k], dev_x)

    def over_y(k, half):
        return remote(pieces(k, of_x, half), pieces(k, of_x, half), yd_s.at[k], yd_r.at[k], dev_y)

    def to_core_x(k, blk):
        return remote(pieces(k, blk, y), pieces(k, blk, y), c3_s.at[k], c3_r.at[k], dev_c)

    def to_core_y(k, blk):
        return remote(pieces(k, blk, oy), pieces(k, blk, oy), c4_s.at[k], c4_r.at[k], dev_c)

    route_devs = (dev_c, dev_x, dev_xc)
    for i in range(3):
        route_copy(i, route_devs[i], ep).start()
    for k in range(len(CHUNKS)):
        over_x(k, own).start()
    for k in range(len(CHUNKS)):
        to_core_own(k, own).start()

    def relay_x(k):
        with jax.named_scope("relay_x"):
            over_x(k, of_x).wait_recv()
        if not CHUNKS[k][2]:
            over_y(k, y).start()
        to_core_x(k, of_x).start()

    def relay_y(k):
        with jax.named_scope("relay_y"):
            over_y(k, oy).wait_recv()
        to_core_y(k, of_x).start()

    with jax.named_scope("route_wait"):
        for i, b in enumerate((2 * x + oc, 2 * ox + c, 2 * ox + oc)):
            route_copy(i, route_devs[i], b).wait_recv()

    def route_row(j):
        return jnp.concatenate([route[b, j:j + 1, :] for b in range(4)], axis=1)

    row_code = (route_row(0), route_row(1))
    row_gate = (route_row(2), route_row(3))
    for e in range(2):
        slot = (lax.broadcasted_iota(jnp.int32, (cap, 4 * rows), 0) + (2 * ep + e) * cap).astype(F32)
        hit0, hit1 = row_code[0] == slot, row_code[1] == slot
        onehot[e] = jnp.where(hit0 | hit1, 1.0, 0.0).astype(BF16)
        g = jnp.where(hit0, row_gate[0], 0.0) + jnp.where(hit1, row_gate[1], 0.0)
        gate_col[e] = jnp.sum(g, axis=1, keepdims=True)

    def build_comb():
        k = lax.broadcasted_iota(jnp.int32, (rows, 4 * cap_local), 1)
        part = jnp.where(k >= 2 * cap_local, 1, 0)
        k = k - part * (2 * cap_local)
        sub = jnp.where(k >= cap_local, 1, 0)
        k = k - sub * cap_local
        dev_of = jnp.where(part == 0, ep, 2 * x + oc)
        with jax.named_scope("comb_mat"):
            for b in range(4):
                slot = ((2 * dev_of + sub) * cap + b * cap_local + k).astype(F32)
                back = jnp.concatenate([route[b]] * 16, axis=0).T
                hit = (back[:, 0:1] == slot) | (back[:, 1:2] == slot)
                one = jnp.where(hit, 1.0, 0.0).astype(BF16)
                comb[b] = jnp.concatenate([one, one, one], axis=1)

    relay_x(0)
    build_comb()
    relay_x(1)
    after = {(0, 1): [(relay_x, 2)],
             (1, 1): [(relay_x, 3), (relay_y, 2), (relay_x, 4)],
             (2, 0): [(relay_y, 3)], (2, 1): [(relay_y, 4)]}

    def product(k, e):
        first, n, _ = CHUNKS[k]
        w, off = first * PIECE // kw, first * PIECE % kw
        slot = (w % GU_SLOTS) * 2 + e
        width = n * PIECE
        last = k == len(CHUNKS) - 1
        for lo in range(0, d_ff, NB):
            span = slice(lo, min(lo + NB, d_ff))
            part = [jnp.dot(xs[e, :, 0:width], wgu[slot, m, off:off + width, span], preferred_element_type=F32)
                    for m in range(2)]
            if k > 0:
                part = [acc[e, m, :, span] + part[m] for m in range(2)]
            if last:
                act[e, :, span] = (jax.nn.silu(part[0]) * part[1]).astype(BF16)
            else:
                for m in range(2):
                    acc[e, m, :, span] = part[m]

    for k, (first, n, direct) in enumerate(CHUNKS):
        w, off = first * PIECE // kw, first * PIECE % kw
        with jax.named_scope("tok_wait"):
            to_core_own(k, of_c).wait_recv()
            to_core_x(k, of_xc).wait_recv()
            if not direct:
                to_core_y(k, of_xc).wait_recv()
        with jax.named_scope("gu_wait"):
            if off == 0:
                for e in range(2):
                    for m in range(2):
                        gu_copy(w, e, m).wait()
        groups = ((0,), (1,)) if (k, 0) in after else ((0, 1),)
        for gi, group in enumerate(groups):
            @pl.when(always)
            def _(k=k, first=first, n=n, group=group, gi=gi):
                with jax.named_scope("gu_dot"):
                    if gi == 0:
                        for e in range(2):
                            for i in range(n):
                                rows_k = jnp.dot(onehot[e], tok[first + i], preferred_element_type=F32)
                                xs[e, :, i * PIECE:(i + 1) * PIECE] = rows_k.astype(BF16)
                    for e in group:
                        product(k, e)
            for e in group:
                if off + n * PIECE == kw and w + GU_SLOTS < N_W:
                    for m in range(2):
                        gu_copy(w + GU_SLOTS, e, m).start(priority=1)
                for fn, arg in after.get((k, e), ()):
                    fn(arg)

    def dw(u):
        return remote(w_all.at[u, oc], w_recv.at[u], dw_s.at[u], dw_r.at[u], dev_c)

    def f1(u, pos):
        return remote(f1_send.at[u, pos], f1_recv.at[u, pos], f1_s.at[u, pos], f1_r.at[u, pos],
                      dev_y if u in Y_FIRST else dev_x)

    def f2(u):
        return remote(f2_send.at[u], f2_recv.at[u], f2_s.at[u], f2_r.at[u], dev_x if u in Y_FIRST else dev_y)

    def out_cols(core, u):
        return pl.ds(pl.multiple_of(u * uw + core * hu, hu), hu)

    def to_other(u):
        return remote(fin.at[u], out_hbm.at[:, out_cols(c, u)], fo_s.at[u, 0], fo_r.at[u, c], dev_fin)

    def to_core(u):
        return remote(fin.at[u], out_hbm.at[:, out_cols(c, u)], fo_s.at[u, 1], fo_r.at[u, c], dev_c)

    def to_self(u):
        return pltpu.make_async_copy(fin.at[u], out_hbm.at[:, out_cols(c, u)], fo_s.at[u, 1])

    def incoming(u, core):
        return remote(fin.at[u], out_hbm.at[:, out_cols(core, u)], fo_s.at[u, 0], fo_r.at[u, core], dev_fin)

    def down(u):
        slot = u % WD_SLOTS
        with jax.named_scope("wd_wait"):
            for e in range(2):
                wd_copy(u, e).wait()
        with jax.named_scope("wd_dot"):
            for e in range(2):
                out = jnp.dot(act[e], wdn[slot, e], preferred_element_type=F32) * gate_col[e]
                for core in range(2):
                    for b in range(4):
                        w_all[u, core, b, e * cap_local:(e + 1) * cap_local] = (
                            out[b * cap_local:(b + 1) * cap_local, core * hu:(core + 1) * hu])
        dw(u).start()
        if u + WD_SLOTS < N_U:
            for e in range(2):
                wd_copy(u + WD_SLOTS, e).start(priority=1)

    def combine(u):
        with jax.named_scope("dw_wait"):
            dw(u).wait_recv()
        if u in Y_FIRST:
            keep1, send0 = 2 * ox + y, 2 * x + oy
        else:
            keep1, send0 = 2 * x + oy, 2 * ox + y
        with jax.named_scope("comb"):
            for dst, pos, b in ((f1_send, 1, 2 * ox + oy), (f1_send, 0, send0),
                                (f1_keep, 1, keep1), (f1_keep, 0, 2 * x + y)):
                s = jnp.concatenate([w_all[u, c, b], w_recv[u, b]], axis=0)
                hi = s.astype(BF16)
                rest = s - hi.astype(F32)
                mid = rest.astype(BF16)
                lo = (rest - mid.astype(F32)).astype(BF16)
                parts = jnp.concatenate([hi, mid, lo], axis=0)
                dst[u, pos] = jnp.dot(comb[b], parts, preferred_element_type=F32)
    def second(u):
        with jax.named_scope("f1_wait"):
            f1(u, 1).wait_recv()
        f2_send[u] = f1_keep[u, 1] + f1_recv[u, 1]
        f2(u).start()

    def final(u):
        with jax.named_scope("f2_wait"):
            f1(u, 0).wait_recv()
            f2(u).wait_recv()
        fin[u] = (f1_keep[u, 0] + f1_recv[u, 0] + f2_recv[u]).astype(BF16)
        to_other(u).start()

        @pl.when(c == y)
        def _():
            to_self(u).start()

        @pl.when(c != y)
        def _():
            to_core(u).start()

    steps = {"D": down, "C": combine, "S": lambda u: f1(u, 1).start(), "H": lambda u: f1(u, 0).start(),
             "A": second, "B": final}
    for step in ORDER:
        steps[step[0]](int(step[1:]))

    with jax.named_scope("end"):
        for i in range(3):
            route_copy(i, route_devs[i], ep).wait_send()
        for k in range(len(CHUNKS)):
            to_core_own(k, own).wait_send()
            over_x(k, own).wait_send()
            to_core_x(k, of_x).wait_send()
            if not CHUNKS[k][2]:
                over_y(k, y).wait_send()
                to_core_y(k, of_x).wait_send()
        for u in range(N_U):
            dw(u).wait_send()
            f1(u, 0).wait_send()
            f1(u, 1).wait_send()
            f2(u).wait_send()
            to_other(u).wait_send()

            @pl.when(c != y)
            def _(u=u):
                to_core(u).wait_send()

            @pl.when(c == y)
            def _(u=u):
                to_self(u).wait()
    with jax.named_scope("in_wait"):
        for u in range(N_U):
            incoming(u, oc).wait_recv()

            @pl.when(c != y)
            def _(u=u):
                incoming(u, c).wait_recv()


def solution(mesh):
    group = mesh.shape['ep']
    row_spec = P(('dp', 'ep'), None)
    col_spec = P('ep', None, 'etp')
    in_specs = (row_spec, row_spec, row_spec, row_spec, col_spec, col_spec, P('ep', 'etp', None))

    def device_step(hidden, expert_ids, gate_wts, slot_pos, w_gate, w_up, w_down):
        rows, d_model = hidden.shape
        top_k = expert_ids.shape[1]
        local_experts = w_gate.shape[0]
        experts = local_experts * group
        cap_local = ((5 * top_k * rows) // (4 * experts) + 7) // 8 * 8
        cap = group * cap_local
        d_ff = w_gate.shape[2]
        hu = d_model // (2 * N_U)
        kw = d_model // N_W
        n_k = len(CHUNKS)
        any_spec = pl.BlockSpec(memory_space=pl.ANY)
        vmem_spec = pl.BlockSpec(memory_space=pltpu.VMEM)
        dma = pltpu.SemaphoreType.DMA
        scratch = [
            pltpu.VMEM((d_model // PIECE, group * rows, PIECE), BF16),
            pltpu.VMEM((group, 8, 128), F32),
            pltpu.VMEM((2, cap, group * rows), BF16),
            pltpu.VMEM((group, rows, 12 * cap_local), BF16),
            pltpu.VMEM((2, cap, 1), F32),
            pltpu.VMEM((2, cap, 2 * PIECE), BF16),
            pltpu.VMEM((2, 2, cap, d_ff), F32),
            pltpu.VMEM((2, cap, d_ff), BF16),
            pltpu.VMEM((2 * GU_SLOTS, 2, kw, d_ff), BF16),
            pltpu.VMEM((WD_SLOTS, 2, d_ff, 2 * hu), BF16),
            pltpu.VMEM((N_U, 2, 4, 2 * cap_local, hu), F32),
            pltpu.VMEM((N_U, 4, 2 * cap_local, hu), F32),
            pltpu.VMEM((N_U, 2, rows, hu), F32),
            pltpu.VMEM((N_U, 2, rows, hu), F32),
            pltpu.VMEM((N_U, 2, rows, hu), F32),
            pltpu.VMEM((N_U, rows, hu), F32),
            pltpu.VMEM((N_U, rows, hu), F32),
            pltpu.VMEM((N_U, rows, hu), BF16),
            dma((d_model // PIECE,)), dma((2 * GU_SLOTS, 2)), dma((WD_SLOTS, 2)),
            dma((3,)), dma((3,)),
        ] + [dma((n_k,))] * 10 + [dma((N_U,))] * 2 + [dma((N_U, 2))] * 2 + [dma((N_U,))] * 2 + [dma((N_U, 2))] * 2
        return pl.pallas_call(
            functools.partial(moe_kernel, rows, d_model, d_ff, cap_local),
            out_shape=jax.ShapeDtypeStruct((rows, d_model), BF16),
            in_specs=[any_spec, vmem_spec, vmem_spec, vmem_spec, any_spec, any_spec, any_spec],
            out_specs=any_spec,
            scratch_shapes=scratch,
            compiler_params=pltpu.CompilerParams(collective_id=0, has_side_effects=True,
                                                 vmem_limit_bytes=67_043_328),
        )(hidden, expert_ids.T, gate_wts.T, slot_pos.T, w_gate, w_up, w_down)

    return jax.shard_map(device_step, mesh=mesh, in_specs=in_specs, out_specs=row_spec, check_vma=False)
```

```python
import functools
import jax
import jax.numpy as jnp
from jax import lax
from jax.sharding import PartitionSpec as P
from jax.experimental import pallas as pl
from jax.experimental.pallas import tpu as pltpu

MESH = pl.DeviceIdType.MESH
F32, BF16 = jnp.float32, jnp.bfloat16
N_W = 4
GU_SLOTS = 3
WD_SLOTS = 3
N_U = 8
NB = 512
PIECE = 256
Y_FIRST = (1, 3, 7)
ORDER = (
    "D0", "D1", "D2", "C0", "S0", "C1", "S1", "H0", "H1", "D3", "C2", "D4",
    "D5", "S2", "C3", "S3", "H2", "D6", "D7", "H3", "C5", "A0", "S5", "C4",
    "C6", "C7", "S7", "S6", "S4", "H5", "H7", "A2", "A3", "H6", "A1", "A6",
    "H4", "A5", "A4", "B2", "B6", "A7", "B0", "B5", "B1", "B4", "B3", "B7",
)


def moe_kernel(rows, d_model, d_ff, cap_local,
               hid_hbm, ids_hbm, gates_hbm, pos_hbm, wg_hbm, wu_hbm, wd_hbm, out_ref,
               ids, gates, pos, tok, route, onehot, comb, gate_col, xs, acc, act, wgu, wdn,
               w_all, w_recv, f1_keep, f1_send, f1_recv, f2_send, f2_recv, fin,
               in_sem, hid_sem, gu_sem, wd_sem, rt_s, rt_r, s1_s, s1_r, xd_s, xd_r, c3_s, c3_r,
               dw_s, dw_r, f1_s, f1_r, f2_s, f2_r, fo_s, fo_r):
    cap = 4 * cap_local
    kw = d_model // N_W
    uw = d_model // N_U
    hu = uw // 2
    n_k = d_model // PIECE
    ep = lax.axis_index("ep")
    y = lax.axis_index("etp")
    c = lax.rem(ep, 2)
    x = ep // 2
    ox, oy, oc = 1 - x, 1 - y, 1 - c
    dev_c = {"ep": 2 * x + oc}
    dev_x = {"ep": 2 * ox + c}
    dev_xc = {"ep": 2 * ox + oc}
    dev_y = {"etp": oy}
    dev_yc = {"etp": oy, "ep": 2 * x + oc}
    dev_fin = {"etp": oy, "ep": 2 * x + y}
    always = ep >= 0

    def remote(src, dst, s, r, dev):
        return pltpu.make_async_remote_copy(src_ref=src, dst_ref=dst, send_sem=s, recv_sem=r,
                                            device_id=dev, device_id_type=MESH)

    def block(b):
        return pl.ds(pl.multiple_of(b * rows, rows), rows)

    own, of_c, of_x, of_xc = block(ep), block(2 * x + oc), block(2 * ox + c), block(2 * ox + oc)

    barrier = pltpu.get_barrier_semaphore()
    for dev in (dev_c, dev_x, dev_xc, dev_y, dev_yc):
        pl.semaphore_signal(barrier, inc=1, device_id=dev, device_id_type=MESH)

    def hid_copy(i):
        return pltpu.make_async_copy(hid_hbm.at[:, i * PIECE:(i + 1) * PIECE], tok.at[i, own], hid_sem)

    hid_all = pltpu.make_async_copy(tok.at[:, own], tok.at[:, own], hid_sem)

    def gu_copy(w, e, m):
        slot = w % GU_SLOTS
        src = (wg_hbm, wu_hbm)[m]
        return pltpu.make_async_copy(src.at[e, pl.ds(w * kw, kw)], wgu.at[slot, e, m], gu_sem.at[slot])

    def gu_all(w):
        slot = w % GU_SLOTS
        return pltpu.make_async_copy(wgu.at[slot], wgu.at[slot], gu_sem.at[slot])

    def wd_copy(u):
        slot = u % WD_SLOTS
        return pltpu.make_async_copy(wd_hbm.at[:, :, pl.ds(u * uw, uw)], wdn.at[slot], wd_sem.at[slot])

    route_in = [pltpu.make_async_copy(src, dst, in_sem.at[i])
                for i, (src, dst) in enumerate(((ids_hbm, ids), (gates_hbm, gates), (pos_hbm, pos)))]
    for cp in route_in:
        cp.start()
    for i in range(n_k):
        hid_copy(i).start()

    for cp in route_in:
        cp.wait()
    code = jnp.where(pos[...] >= 0, ids[...] * cap + pos[...], -1).astype(F32)
    route[ep] = jnp.concatenate([code, gates[...], jnp.zeros((4, rows), F32)], axis=0)
    with jax.named_scope("hid_wait"):
        hid_all.wait()
    for w in range(GU_SLOTS):
        for e in range(2):
            for m in range(2):
                gu_copy(w, e, m).start(priority=1)
    with jax.named_scope("barrier"):
        pl.semaphore_wait(barrier, 5)

    def route_copy(i, b):
        return remote(route.at[b], route.at[b], rt_s, rt_r, route_devs[i])

    route_all = remote(route.at[pl.ds(0, 3)], route.at[pl.ds(0, 3)], rt_s, rt_r, dev_c)

    def to_core_own(k, blk):
        return remote(tok.at[k, blk], tok.at[k, blk], s1_s, s1_r, dev_c)

    def over_x(k, blk):
        return remote(tok.at[k, blk], tok.at[k, blk], xd_s, xd_r.at[k], dev_x)

    def to_core_x(k, blk):
        return remote(tok.at[k, blk], tok.at[k, blk], c3_s, c3_r.at[k], dev_c)

    route_devs = (dev_c, dev_x, dev_xc)
    for i in range(3):
        route_copy(i, ep).start()
    for k in range(n_k):
        over_x(k, own).start()
    for k in range(n_k):
        to_core_own(k, own).start()

    def relay_x(k):
        with jax.named_scope("relay_x"):
            over_x(k, of_x).wait_recv()
        to_core_x(k, of_x).start()

    with jax.named_scope("route_wait"):
        route_all.wait_recv()

    def route_row(j):
        return jnp.concatenate([route[b, j:j + 1, :] for b in range(4)], axis=1)

    row_code = (route_row(0), route_row(1))
    row_gate = (route_row(2), route_row(3))
    for e in range(2):
        slot = (lax.broadcasted_iota(jnp.int32, (cap, 4 * rows), 0) + (2 * ep + e) * cap).astype(F32)
        hit0, hit1 = row_code[0] == slot, row_code[1] == slot
        onehot[e] = jnp.where(hit0 | hit1, 1.0, 0.0).astype(BF16)
        g = jnp.where(hit0, row_gate[0], 0.0) + jnp.where(hit1, row_gate[1], 0.0)
        gate_col[e] = jnp.sum(g, axis=1, keepdims=True)

    def build_comb():
        k = lax.broadcasted_iota(jnp.int32, (rows, 4 * cap_local), 1)
        part = jnp.where(k >= 2 * cap_local, 1, 0)
        k = k - part * (2 * cap_local)
        sub = jnp.where(k >= cap_local, 1, 0)
        k = k - sub * cap_local
        dev_of = jnp.where(part == 0, ep, 2 * x + oc)
        with jax.named_scope("comb_mat"):
            for b in range(4):
                slot = ((2 * dev_of + sub) * cap + b * cap_local + k).astype(F32)
                back = jnp.concatenate([route[b]] * 16, axis=0).T
                hit = (back[:, 0:1] == slot) | (back[:, 1:2] == slot)
                one = jnp.where(hit, 1.0, 0.0).astype(BF16)
                comb[b] = jnp.concatenate([one, one, one], axis=1)

    def product(k, e):
        w, off = k * PIECE // kw, k * PIECE % kw
        slot = w % GU_SLOTS
        for lo in range(0, d_ff, NB):
            span = slice(lo, min(lo + NB, d_ff))
            part = [jnp.dot(xs[e], wgu[slot, e, m, off:off + PIECE, span], preferred_element_type=F32)
                    for m in range(2)]
            if k > 0:
                part = [acc[e, m, :, span] + part[m] for m in range(2)]
            if k == n_k - 1:
                act[e, :, span] = (jax.nn.silu(part[0]) * part[1]).astype(BF16)
            else:
                for m in range(2):
                    acc[e, m, :, span] = part[m]

    relay_x(0)
    build_comb()
    relay_x(1)
    with jax.named_scope("tok_wait"):
        remote(tok.at[:, of_c], tok.at[:, of_c], s1_s, s1_r, dev_c).wait_recv()
    for k in range(n_k):
        w, off = k * PIECE // kw, k * PIECE % kw
        with jax.named_scope("tok_wait"):
            to_core_x(k, of_xc).wait_recv()
        if off == 0:
            with jax.named_scope("gu_wait"):
                gu_all(w).wait()

        @pl.when(always)
        def _(k=k):
            with jax.named_scope("gu_dot"):
                for e in range(2):
                    xs[e] = jnp.dot(onehot[e], tok[k], preferred_element_type=F32).astype(BF16)
                for e in range(2):
                    product(k, e)

        if off + PIECE == kw and w + GU_SLOTS < N_W:
            for e in range(2):
                for m in range(2):
                    gu_copy(w + GU_SLOTS, e, m).start(priority=1)
        if k == n_k - 3:
            for u in range(WD_SLOTS):
                wd_copy(u).start(priority=1)
        if k + 2 < n_k:
            relay_x(k + 2)

    def dw(u):
        return remote(w_all.at[u, oc], w_recv.at[u], dw_s, dw_r.at[u], dev_c)

    def f1(u, pos):
        return remote(f1_send.at[u, pos], f1_recv.at[u, pos], f1_s, f1_r.at[u, pos],
                      dev_y if u in Y_FIRST else dev_x)

    def f2(u):
        return remote(f2_send.at[u], f2_recv.at[u], f2_s, f2_r.at[u], dev_x if u in Y_FIRST else dev_y)

    def out_cols(core, u):
        return pl.ds(pl.multiple_of(u * uw + core * hu, hu), hu)

    def to_other(u):
        return remote(fin.at[u], out_ref.at[:, out_cols(c, u)], fo_s.at[0], fo_r.at[c], dev_fin)

    def to_core(u):
        return remote(fin.at[u], out_ref.at[:, out_cols(c, u)], fo_s.at[1], fo_r.at[c], dev_c)

    def down(u):
        slot = u % WD_SLOTS
        with jax.named_scope("wd_wait"):
            wd_copy(u).wait()
        with jax.named_scope("wd_dot"):
            for e in range(2):
                out = jnp.dot(act[e], wdn[slot, e], preferred_element_type=F32) * gate_col[e]
                for core in range(2):
                    for b in range(4):
                        w_all[u, core, b, e * cap_local:(e + 1) * cap_local] = (
                            out[b * cap_local:(b + 1) * cap_local, core * hu:(core + 1) * hu])
        dw(u).start()
        if u + WD_SLOTS < N_U:
            wd_copy(u + WD_SLOTS).start(priority=1)

    def combine(u):
        with jax.named_scope("dw_wait"):
            dw(u).wait_recv()
        if u in Y_FIRST:
            keep1, send0 = 2 * ox + y, 2 * x + oy
        else:
            keep1, send0 = 2 * x + oy, 2 * ox + y
        with jax.named_scope("comb"):
            for dst, pos, b in ((f1_send, 1, 2 * ox + oy), (f1_send, 0, send0),
                                (f1_keep, 1, keep1), (f1_keep, 0, 2 * x + y)):
                s = jnp.concatenate([w_all[u, c, b], w_recv[u, b]], axis=0)
                hi = s.astype(BF16)
                rest = s - hi.astype(F32)
                mid = rest.astype(BF16)
                lo = (rest - mid.astype(F32)).astype(BF16)
                parts = jnp.concatenate([hi, mid, lo], axis=0)
                dst[u, pos] = jnp.dot(comb[b], parts, preferred_element_type=F32)
    def second(u):
        with jax.named_scope("f1_wait"):
            f1(u, 1).wait_recv()
        f2_send[u] = f1_keep[u, 1] + f1_recv[u, 1]
        f2(u).start()

    def final(u):
        with jax.named_scope("f2_wait"):
            f1(u, 0).wait_recv()
            f2(u).wait_recv()
        fin[u] = (f1_keep[u, 0] + f1_recv[u, 0] + f2_recv[u]).astype(BF16)
        to_other(u).start()

        @pl.when(c == y)
        def _():
            out_ref[:, out_cols(c, u)] = fin[u]

        @pl.when(c != y)
        def _():
            to_core(u).start()

    steps = {"D": down, "C": combine, "S": lambda u: f1(u, 1).start(), "H": lambda u: f1(u, 0).start(),
             "A": second, "B": final}
    for step in ORDER:
        steps[step[0]](int(step[1:]))

    with jax.named_scope("end"):
        route_all.wait_send()
        remote(tok.at[:, own], tok.at[:, own], s1_s, s1_r, dev_c).wait_send()
        remote(tok.at[:, own], tok.at[:, own], xd_s, xd_r.at[0], dev_x).wait_send()
        remote(tok.at[:, of_x], tok.at[:, of_x], c3_s, c3_r.at[0], dev_c).wait_send()
        remote(w_all.at[:, oc], w_recv, dw_s, dw_r.at[0], dev_c).wait_send()
        remote(f1_send, f1_recv, f1_s, f1_r.at[0, 0], dev_x).wait_send()
        remote(f2_send, f2_recv, f2_s, f2_r.at[0], dev_y).wait_send()
        remote(fin, fin, fo_s.at[0], fo_r.at[0], dev_fin).wait_send()

        @pl.when(c != y)
        def _():
            remote(fin, fin, fo_s.at[1], fo_r.at[0], dev_c).wait_send()
    with jax.named_scope("in_wait"):
        remote(fin, fin, fo_s.at[0], fo_r.at[oc], dev_fin).wait_recv()

        @pl.when(c != y)
        def _():
            remote(fin, fin, fo_s.at[0], fo_r.at[c], dev_fin).wait_recv()


def solution(mesh):
    group = mesh.shape['ep']
    row_spec = P(('dp', 'ep'), None)
    col_spec = P('ep', None, 'etp')
    in_specs = (row_spec, row_spec, row_spec, row_spec, col_spec, col_spec, P('ep', 'etp', None))

    def device_step(hidden, expert_ids, gate_wts, slot_pos, w_gate, w_up, w_down):
        rows, d_model = hidden.shape
        top_k = expert_ids.shape[1]
        local_experts = w_gate.shape[0]
        experts = local_experts * group
        cap_local = ((5 * top_k * rows) // (4 * experts) + 7) // 8 * 8
        cap = group * cap_local
        d_ff = w_gate.shape[2]
        hu = d_model // (2 * N_U)
        kw = d_model // N_W
        n_k = d_model // PIECE
        any_spec = pl.BlockSpec(memory_space=pl.ANY)
        vmem_spec = pl.BlockSpec(memory_space=pltpu.VMEM)
        dma = pltpu.SemaphoreType.DMA
        scratch = [
            pltpu.VMEM((top_k, rows), jnp.int32),
            pltpu.VMEM((top_k, rows), F32),
            pltpu.VMEM((top_k, rows), jnp.int32),
            pltpu.VMEM((d_model // PIECE, group * rows, PIECE), BF16),
            pltpu.VMEM((group, 8, 128), F32),
            pltpu.VMEM((2, cap, group * rows), BF16),
            pltpu.VMEM((group, rows, 12 * cap_local), BF16),
            pltpu.VMEM((2, cap, 1), F32),
            pltpu.VMEM((2, cap, PIECE), BF16),
            pltpu.VMEM((2, 2, cap, d_ff), F32),
            pltpu.VMEM((2, cap, d_ff), BF16),
            pltpu.VMEM((GU_SLOTS, 2, 2, kw, d_ff), BF16),
            pltpu.VMEM((WD_SLOTS, 2, d_ff, 2 * hu), BF16),
            pltpu.VMEM((N_U, 2, 4, 2 * cap_local, hu), F32),
            pltpu.VMEM((N_U, 4, 2 * cap_local, hu), F32),
            pltpu.VMEM((N_U, 2, rows, hu), F32),
            pltpu.VMEM((N_U, 2, rows, hu), F32),
            pltpu.VMEM((N_U, 2, rows, hu), F32),
            pltpu.VMEM((N_U, rows, hu), F32),
            pltpu.VMEM((N_U, rows, hu), F32),
            pltpu.VMEM((N_U, rows, hu), BF16),
            dma((3,)), dma, dma((GU_SLOTS,)), dma((WD_SLOTS,)), dma, dma, dma, dma,
            dma, dma((n_k,)), dma, dma((n_k,)),
            dma, dma((N_U,)), dma, dma((N_U, 2)), dma, dma((N_U,)), dma((2,)), dma((2,)),
        ]
        return pl.pallas_call(
            functools.partial(moe_kernel, rows, d_model, d_ff, cap_local),
            out_shape=pltpu.VMEM((rows, d_model), BF16),
            in_specs=[any_spec] * 7,
            out_specs=vmem_spec,
            scratch_shapes=scratch,
            compiler_params=pltpu.CompilerParams(collective_id=0, has_side_effects=True,
                                                 vmem_limit_bytes=66_400_000),
        )(hidden, expert_ids.T, gate_wts.T, slot_pos.T, w_gate, w_up, w_down)

    return jax.shard_map(device_step, mesh=mesh, in_specs=in_specs, out_specs=row_spec, check_vma=False)
```

```python
import functools
import jax
import jax.numpy as jnp
from jax import lax
from jax.sharding import PartitionSpec as P
from jax.experimental import pallas as pl
from jax.experimental.pallas import tpu as pltpu

MESH = pl.DeviceIdType.MESH
F32, BF16 = jnp.float32, jnp.bfloat16
N_W = 4
GU_SLOTS = 3
WD_SLOTS = 3
N_U = 8
NB = 512
PIECE = 256
Y_FIRST = (0, 3, 5)
AT_ONCE = (0, 1, 2, 3, 4)
ORDER = (
    "D0", "D1", "D2", "C0", "S0", "C1", "S1", "D3", "H0", "C2", "S2", "D4",
    "C3", "S3", "H3", "H1", "D5", "H2", "D6", "C4", "S4", "D7", "A1", "C5",
    "C6", "C7", "S6", "A2", "S5", "S7", "A3", "B1", "H7", "A6", "H6", "A5",
    "H5", "A7", "A4", "B3", "H4", "B2", "A0", "B6", "B5", "B4", "B7", "B0",
)


def moe_kernel(rows, d_model, d_ff, cap_local,
               hid_hbm, ids_hbm, gates_hbm, pos_hbm, wg_hbm, wu_hbm, wd_hbm, out_ref,
               ids, gates, pos, tok, route, onehot, comb, gate_col, xs, acc, act, wgu, wdn,
               w_all, w_recv, f1_keep, f1_send, f1_recv, f2_send, f2_recv, fin,
               in_sem, hid_sem, gu_sem, wd_sem, rt_s, rt_r, s1_s, s1_r, xd_s, xd_r, c3_s, c3_r,
               dw_s, dw_r, f1_s, f1_r, f2_s, f2_r, fo_s, fo_r):
    cap = 4 * cap_local
    kw = d_model // N_W
    uw = d_model // N_U
    hu = uw // 2
    n_k = d_model // PIECE
    ep = lax.axis_index("ep")
    y = lax.axis_index("etp")
    c = lax.rem(ep, 2)
    x = ep // 2
    ox, oy, oc = 1 - x, 1 - y, 1 - c
    dev_c = {"ep": 2 * x + oc}
    dev_x = {"ep": 2 * ox + c}
    dev_xc = {"ep": 2 * ox + oc}
    dev_y = {"etp": oy}
    dev_yc = {"etp": oy, "ep": 2 * x + oc}
    dev_fin = {"etp": oy, "ep": 2 * x + y}
    always = ep >= 0

    def remote(src, dst, s, r, dev):
        return pltpu.make_async_remote_copy(src_ref=src, dst_ref=dst, send_sem=s, recv_sem=r,
                                            device_id=dev, device_id_type=MESH)

    def block(b):
        return pl.ds(pl.multiple_of(b * rows, rows), rows)

    own, of_c, of_x, of_xc = block(ep), block(2 * x + oc), block(2 * ox + c), block(2 * ox + oc)

    barrier = pltpu.get_barrier_semaphore()
    for dev in (dev_c, dev_x, dev_xc, dev_y, dev_yc):
        pl.semaphore_signal(barrier, inc=1, device_id=dev, device_id_type=MESH)

    def hid_copy(i):
        return pltpu.make_async_copy(hid_hbm.at[:, i * PIECE:(i + 1) * PIECE], tok.at[i, own], hid_sem)

    hid_all = pltpu.make_async_copy(tok.at[:, own], tok.at[:, own], hid_sem)

    def gu_copy(w, e, m):
        slot = w % GU_SLOTS
        src = (wg_hbm, wu_hbm)[m]
        return pltpu.make_async_copy(src.at[e, pl.ds(w * kw, kw)], wgu.at[slot, e, m], gu_sem.at[slot])

    def gu_all(w):
        slot = w % GU_SLOTS
        return pltpu.make_async_copy(wgu.at[slot], wgu.at[slot], gu_sem.at[slot])

    def wd_copy(u):
        slot = u % WD_SLOTS
        return pltpu.make_async_copy(wd_hbm.at[:, :, pl.ds(u * uw, uw)], wdn.at[slot], wd_sem.at[slot])

    route_in = [pltpu.make_async_copy(src, dst, in_sem.at[i])
                for i, (src, dst) in enumerate(((ids_hbm, ids), (gates_hbm, gates), (pos_hbm, pos)))]
    for cp in route_in:
        cp.start()
    for i in range(n_k):
        hid_copy(i).start()
    for w in range(GU_SLOTS):
        for e in range(2):
            for m in range(2):
                gu_copy(w, e, m).start(priority=1)

    for cp in route_in:
        cp.wait()
    code = jnp.where(pos[...] >= 0, ids[...] * cap + pos[...], -1).astype(F32)
    route[ep] = jnp.concatenate([code, gates[...], jnp.zeros((4, rows), F32)], axis=0)
    with jax.named_scope("hid_wait"):
        hid_all.wait()
    with jax.named_scope("barrier"):
        pl.semaphore_wait(barrier, 5)

    def route_copy(i, b):
        return remote(route.at[b], route.at[b], rt_s, rt_r, route_devs[i])

    route_all = remote(route.at[pl.ds(0, 3)], route.at[pl.ds(0, 3)], rt_s, rt_r, dev_c)

    def to_core_own(k, blk):
        return remote(tok.at[k, blk], tok.at[k, blk], s1_s, s1_r, dev_c)

    def over_x(k, blk):
        return remote(tok.at[k, blk], tok.at[k, blk], xd_s, xd_r.at[k], dev_x)

    def to_core_x(k, blk):
        return remote(tok.at[k, blk], tok.at[k, blk], c3_s, c3_r.at[k], dev_c)

    route_devs = (dev_c, dev_x, dev_xc)
    for i in range(3):
        route_copy(i, ep).start()
    for k in range(n_k):
        over_x(k, own).start()
    for k in range(n_k):
        to_core_own(k, own).start()

    def relay_x(k):
        with jax.named_scope("relay_x"):
            over_x(k, of_x).wait_recv()
        to_core_x(k, of_x).start()

    with jax.named_scope("route_wait"):
        route_all.wait_recv()

    def route_row(j):
        return jnp.concatenate([route[b, j:j + 1, :] for b in range(4)], axis=1)

    row_code = (route_row(0), route_row(1))
    row_gate = (route_row(2), route_row(3))
    for e in range(2):
        slot = (lax.broadcasted_iota(jnp.int32, (cap, 4 * rows), 0) + (2 * ep + e) * cap).astype(F32)
        hit0, hit1 = row_code[0] == slot, row_code[1] == slot
        onehot[e] = jnp.where(hit0 | hit1, 1.0, 0.0).astype(BF16)
        g = jnp.where(hit0, row_gate[0], 0.0) + jnp.where(hit1, row_gate[1], 0.0)
        gate_col[e] = jnp.sum(g, axis=1, keepdims=True)

    def build_comb():
        k = lax.broadcasted_iota(jnp.int32, (rows, 4 * cap_local), 1)
        part = jnp.where(k >= 2 * cap_local, 1, 0)
        k = k - part * (2 * cap_local)
        sub = jnp.where(k >= cap_local, 1, 0)
        k = k - sub * cap_local
        dev_of = jnp.where(part == 0, ep, 2 * x + oc)
        with jax.named_scope("comb_mat"):
            for b in range(4):
                slot = ((2 * dev_of + sub) * cap + b * cap_local + k).astype(F32)
                back = jnp.concatenate([route[b]] * 16, axis=0).T
                hit = (back[:, 0:1] == slot) | (back[:, 1:2] == slot)
                one = jnp.where(hit, 1.0, 0.0).astype(BF16)
                comb[b] = jnp.concatenate([one, one, one], axis=1)

    def product(k, e):
        w, off = k * PIECE // kw, k * PIECE % kw
        slot = w % GU_SLOTS
        for lo in range(0, d_ff, NB):
            span = slice(lo, min(lo + NB, d_ff))
            part = [jnp.dot(xs[e], wgu[slot, e, m, off:off + PIECE, span], preferred_element_type=F32)
                    for m in range(2)]
            if k > 0:
                part = [acc[e, m, :, span] + part[m] for m in range(2)]
            if k == n_k - 1:
                act[e, :, span] = (jax.nn.silu(part[0]) * part[1]).astype(BF16)
            else:
                for m in range(2):
                    acc[e, m, :, span] = part[m]

    relay_x(0)
    build_comb()
    relay_x(1)
    with jax.named_scope("tok_wait"):
        remote(tok.at[:, of_c], tok.at[:, of_c], s1_s, s1_r, dev_c).wait_recv()
    for k in range(n_k):
        w, off = k * PIECE // kw, k * PIECE % kw
        with jax.named_scope("tok_wait"):
            to_core_x(k, of_xc).wait_recv()
        if off == 0:
            with jax.named_scope("gu_wait"):
                gu_all(w).wait()

        @pl.when(always)
        def _(k=k):
            with jax.named_scope("gu_dot"):
                for e in range(2):
                    xs[e] = jnp.dot(onehot[e], tok[k], preferred_element_type=F32).astype(BF16)
                for e in range(2):
                    product(k, e)

        if off + PIECE == kw and w + GU_SLOTS < N_W:
            for e in range(2):
                for m in range(2):
                    gu_copy(w + GU_SLOTS, e, m).start(priority=1)
        if k == n_k - 3:
            for u in range(WD_SLOTS):
                wd_copy(u).start(priority=1)
        if k + 2 < n_k:
            relay_x(k + 2)

    def dw(u):
        return remote(w_all.at[u, oc], w_recv.at[u], dw_s, dw_r.at[u], dev_c)

    def f1(u, pos):
        return remote(f1_send.at[u, pos], f1_recv.at[u, pos], f1_s, f1_r.at[u, pos],
                      dev_y if u in Y_FIRST else dev_x)

    def f2(u):
        return remote(f2_send.at[u], f2_recv.at[u], f2_s, f2_r.at[u], dev_x if u in Y_FIRST else dev_y)

    def out_cols(core, u):
        return pl.ds(pl.multiple_of(u * uw + core * hu, hu), hu)

    def to_other(u):
        return remote(fin.at[u], out_ref.at[:, out_cols(c, u)], fo_s.at[0], fo_r.at[c], dev_fin)

    def to_core(u):
        return remote(fin.at[u], out_ref.at[:, out_cols(c, u)], fo_s.at[1], fo_r.at[c], dev_c)

    def down(u):
        slot = u % WD_SLOTS
        with jax.named_scope("wd_wait"):
            wd_copy(u).wait()
        with jax.named_scope("wd_dot"):
            for e in range(2):
                out = jnp.dot(act[e], wdn[slot, e], preferred_element_type=F32) * gate_col[e]
                for core in range(2):
                    for b in range(4):
                        w_all[u, core, b, e * cap_local:(e + 1) * cap_local] = (
                            out[b * cap_local:(b + 1) * cap_local, core * hu:(core + 1) * hu])
        dw(u).start()
        if u + WD_SLOTS < N_U:
            wd_copy(u + WD_SLOTS).start(priority=1)

    def combine(u):
        with jax.named_scope("dw_wait"):
            dw(u).wait_recv()
        if u in Y_FIRST:
            keep1, send0 = 2 * ox + y, 2 * x + oy
        else:
            keep1, send0 = 2 * x + oy, 2 * ox + y
        with jax.named_scope("comb"):
            for dst, pos, b in ((f1_send, 1, 2 * ox + oy), (f1_send, 0, send0),
                                (f1_keep, 1, keep1), (f1_keep, 0, 2 * x + y)):
                s = jnp.concatenate([w_all[u, c, b], w_recv[u, b]], axis=0)
                hi = s.astype(BF16)
                rest = s - hi.astype(F32)
                mid = rest.astype(BF16)
                lo = (rest - mid.astype(F32)).astype(BF16)
                parts = jnp.concatenate([hi, mid, lo], axis=0)
                dst[u, pos] = jnp.dot(comb[b], parts, preferred_element_type=F32)
                if dst is f1_send and pos == 1 and u in AT_ONCE:
                    f1(u, 1).start()
    def second(u):
        with jax.named_scope("f1_wait"):
            f1(u, 1).wait_recv()
        f2_send[u] = f1_keep[u, 1] + f1_recv[u, 1]
        f2(u).start()

    def final(u):
        with jax.named_scope("f2_wait"):
            f1(u, 0).wait_recv()
            f2(u).wait_recv()
        fin[u] = (f1_keep[u, 0] + f1_recv[u, 0] + f2_recv[u]).astype(BF16)
        to_other(u).start()

        @pl.when(c == y)
        def _():
            out_ref[:, out_cols(c, u)] = fin[u]

        @pl.when(c != y)
        def _():
            to_core(u).start()

    steps = {"D": down, "C": combine, "S": lambda u: None if u in AT_ONCE else f1(u, 1).start(), "H": lambda u: f1(u, 0).start(),
             "A": second, "B": final}
    for step in ORDER:
        steps[step[0]](int(step[1:]))

    with jax.named_scope("end"):
        route_all.wait_send()
        remote(tok.at[:, own], tok.at[:, own], s1_s, s1_r, dev_c).wait_send()
        remote(tok.at[:, own], tok.at[:, own], xd_s, xd_r.at[0], dev_x).wait_send()
        remote(tok.at[:, of_x], tok.at[:, of_x], c3_s, c3_r.at[0], dev_c).wait_send()
        remote(w_all.at[:, oc], w_recv, dw_s, dw_r.at[0], dev_c).wait_send()
        remote(f1_send, f1_recv, f1_s, f1_r.at[0, 0], dev_x).wait_send()
        remote(f2_send, f2_recv, f2_s, f2_r.at[0], dev_y).wait_send()
        remote(fin, fin, fo_s.at[0], fo_r.at[0], dev_fin).wait_send()

        @pl.when(c != y)
        def _():
            remote(fin, fin, fo_s.at[1], fo_r.at[0], dev_c).wait_send()
    with jax.named_scope("in_wait"):
        remote(fin, fin, fo_s.at[0], fo_r.at[oc], dev_fin).wait_recv()

        @pl.when(c != y)
        def _():
            remote(fin, fin, fo_s.at[0], fo_r.at[c], dev_fin).wait_recv()


def solution(mesh):
    group = mesh.shape['ep']
    row_spec = P(('dp', 'ep'), None)
    col_spec = P('ep', None, 'etp')
    in_specs = (row_spec, row_spec, row_spec, row_spec, col_spec, col_spec, P('ep', 'etp', None))

    def device_step(hidden, expert_ids, gate_wts, slot_pos, w_gate, w_up, w_down):
        rows, d_model = hidden.shape
        top_k = expert_ids.shape[1]
        local_experts = w_gate.shape[0]
        experts = local_experts * group
        cap_local = ((5 * top_k * rows) // (4 * experts) + 7) // 8 * 8
        cap = group * cap_local
        d_ff = w_gate.shape[2]
        hu = d_model // (2 * N_U)
        kw = d_model // N_W
        n_k = d_model // PIECE
        any_spec = pl.BlockSpec(memory_space=pl.ANY)
        vmem_spec = pl.BlockSpec(memory_space=pltpu.VMEM)
        dma = pltpu.SemaphoreType.DMA
        scratch = [
            pltpu.VMEM((top_k, rows), jnp.int32),
            pltpu.VMEM((top_k, rows), F32),
            pltpu.VMEM((top_k, rows), jnp.int32),
            pltpu.VMEM((d_model // PIECE, group * rows, PIECE), BF16),
            pltpu.VMEM((group, 8, 128), F32),
            pltpu.VMEM((2, cap, group * rows), BF16),
            pltpu.VMEM((group, rows, 12 * cap_local), BF16),
            pltpu.VMEM((2, cap, 1), F32),
            pltpu.VMEM((2, cap, PIECE), BF16),
            pltpu.VMEM((2, 2, cap, d_ff), F32),
            pltpu.VMEM((2, cap, d_ff), BF16),
            pltpu.VMEM((GU_SLOTS, 2, 2, kw, d_ff), BF16),
            pltpu.VMEM((WD_SLOTS, 2, d_ff, 2 * hu), BF16),
            pltpu.VMEM((N_U, 2, 4, 2 * cap_local, hu), F32),
            pltpu.VMEM((N_U, 4, 2 * cap_local, hu), F32),
            pltpu.VMEM((N_U, 2, rows, hu), F32),
            pltpu.VMEM((N_U, 2, rows, hu), F32),
            pltpu.VMEM((N_U, 2, rows, hu), F32),
            pltpu.VMEM((N_U, rows, hu), F32),
            pltpu.VMEM((N_U, rows, hu), F32),
            pltpu.VMEM((N_U, rows, hu), BF16),
            dma((3,)), dma, dma((GU_SLOTS,)), dma((WD_SLOTS,)), dma, dma, dma, dma,
            dma, dma((n_k,)), dma, dma((n_k,)),
            dma, dma((N_U,)), dma, dma((N_U, 2)), dma, dma((N_U,)), dma((2,)), dma((2,)),
        ]
        return pl.pallas_call(
            functools.partial(moe_kernel, rows, d_model, d_ff, cap_local),
            out_shape=pltpu.VMEM((rows, d_model), BF16),
            in_specs=[any_spec] * 7,
            out_specs=vmem_spec,
            scratch_shapes=scratch,
            compiler_params=pltpu.CompilerParams(collective_id=0, has_side_effects=True,
                                                 vmem_limit_bytes=66_400_000),
        )(hidden, expert_ids.T, gate_wts.T, slot_pos.T, w_gate, w_up, w_down)

    return jax.shard_map(device_step, mesh=mesh, in_specs=in_specs, out_specs=row_spec, check_vma=False)
```

```python
import functools
import jax
import jax.numpy as jnp
from jax import lax
from jax.sharding import PartitionSpec as P
from jax.experimental import pallas as pl
from jax.experimental.pallas import tpu as pltpu

MESH = pl.DeviceIdType.MESH
F32, BF16 = jnp.float32, jnp.bfloat16
N_W = 4
GU_SLOTS = 3
WD_SLOTS = 3
N_U = 8
NB = 256
PIECE = 256
PAIR = 2
Y_FIRST = (1, 3, 5)
AT_ONCE = (0, 1, 3, 7)
ORDER = (
    "D0", "D1", "D2", "C0", "S0", "C1", "S1", "H0", "D3", "C2", "H1", "D4",
    "S2", "C3", "S3", "D5", "H3", "H2", "C4", "D6", "A0", "D7", "S4", "C5",
    "A2", "A1", "S5", "H5", "C6", "C7", "S7", "A4", "A3", "S6", "H7", "A7",
    "A5", "B2", "H4", "B1", "H6", "B0", "A6", "B3", "B7", "B5", "B4", "B6",
)


def moe_kernel(rows, d_model, d_ff, cap_local,
               hid_hbm, ids_hbm, gates_hbm, pos_hbm, wg_hbm, wu_hbm, wd_hbm, out_ref,
               ids, gates, pos, tok, route, onehot, comb, gate_col, xs, acc, act, wgu, wdn,
               w_all, w_recv, f1_keep, f1_send, f1_recv, f2_send, f2_recv, fin,
               in_sem, hid_sem, gu_sem, wd_sem, rt_s, rt_r, s1_s, s1_r, xd_s, xd_r, yd_s, yd_r, c3_s, c3_r,
               dw_s, dw_r, f1_s, f1_r, f2_s, f2_r, fo_s, fo_r):
    cap = 4 * cap_local
    kw = d_model // N_W
    uw = d_model // N_U
    hu = uw // 2
    n_k = d_model // PIECE
    ep = lax.axis_index("ep")
    y = lax.axis_index("etp")
    c = lax.rem(ep, 2)
    x = ep // 2
    ox, oy, oc = 1 - x, 1 - y, 1 - c
    dev_c = {"ep": 2 * x + oc}
    dev_x = {"ep": 2 * ox + c}
    dev_xc = {"ep": 2 * ox + oc}
    dev_y = {"etp": oy}
    dev_yc = {"etp": oy, "ep": 2 * x + oc}
    dev_fin = {"etp": oy, "ep": 2 * x + y}
    always = ep >= 0

    def remote(src, dst, s, r, dev):
        return pltpu.make_async_remote_copy(src_ref=src, dst_ref=dst, send_sem=s, recv_sem=r,
                                            device_id=dev, device_id_type=MESH)

    def block(b):
        return pl.ds(pl.multiple_of(b * rows, rows), rows)

    own, of_c, of_x, of_xc = block(ep), block(2 * x + oc), block(2 * ox + c), block(2 * ox + oc)

    barrier = pltpu.get_barrier_semaphore()
    for dev in (dev_c, dev_x, dev_xc, dev_y, dev_yc):
        pl.semaphore_signal(barrier, inc=1, device_id=dev, device_id_type=MESH)

    def hid_copy(i):
        return pltpu.make_async_copy(hid_hbm.at[:, i * PIECE:(i + 1) * PIECE], tok.at[i, own], hid_sem)

    hid_all = pltpu.make_async_copy(tok.at[:, own], tok.at[:, own], hid_sem)

    def gu_copy(w, e, m):
        slot = w % GU_SLOTS
        src = (wg_hbm, wu_hbm)[m]
        return pltpu.make_async_copy(src.at[e, pl.ds(w * kw, kw)], wgu.at[slot, e, m], gu_sem.at[slot])

    def gu_all(w):
        slot = w % GU_SLOTS
        return pltpu.make_async_copy(wgu.at[slot], wgu.at[slot], gu_sem.at[slot])

    def wd_copy(u):
        slot = u % WD_SLOTS
        return pltpu.make_async_copy(wd_hbm.at[:, :, pl.ds(u * uw, uw)], wdn.at[slot], wd_sem.at[slot])

    route_in = [pltpu.make_async_copy(src, dst, in_sem.at[i])
                for i, (src, dst) in enumerate(((ids_hbm, ids), (gates_hbm, gates), (pos_hbm, pos)))]
    for cp in route_in:
        cp.start()
    for i in range(n_k):
        hid_copy(i).start()
    for w in range(GU_SLOTS):
        for e in range(2):
            for m in range(2):
                gu_copy(w, e, m).start(priority=1)

    for cp in route_in:
        cp.wait()
    code = jnp.where(pos[...] >= 0, ids[...] * cap + pos[...], -1).astype(F32)
    route[ep] = jnp.concatenate([code, gates[...], jnp.zeros((4, rows), F32)], axis=0)
    with jax.named_scope("hid_wait"):
        hid_all.wait()
    with jax.named_scope("barrier"):
        pl.semaphore_wait(barrier, 5)

    def route_copy(i, b):
        return remote(route.at[b], route.at[b], rt_s, rt_r, route_devs[i])

    route_all = remote(route.at[pl.ds(0, 3)], route.at[pl.ds(0, 3)], rt_s, rt_r, dev_c)

    def to_core_own(k, blk):
        return remote(tok.at[k, blk], tok.at[k, blk], s1_s, s1_r, dev_c)

    def over_x(k, blk):
        return remote(tok.at[k, blk], tok.at[k, blk], xd_s, xd_r.at[k], dev_x)

    def to_core_x(k, blk):
        return remote(tok.at[k, blk], tok.at[k, blk], c3_s, c3_r.at[k], dev_c)

    route_devs = (dev_c, dev_x, dev_xc)
    for i in range(3):
        route_copy(i, ep).start()
    mine, other = PAIR + y, PAIR + oy

    def pair_over_x(blk):
        return remote(tok.at[mine, blk], tok.at[mine, blk], xd_s, xd_r.at[PAIR], dev_x)

    def pair_over_y(k):
        return remote(tok.at[k, of_x], tok.at[k, of_x], yd_s, yd_r, dev_y)

    def pair_to_core(k, i, blk):
        return remote(tok.at[k, blk], tok.at[k, blk], c3_s, c3_r.at[PAIR + i], dev_c)

    for k in range(n_k):
        if k == PAIR:
            pair_over_x(own).start()
        elif k != PAIR + 1:
            over_x(k, own).start()
    for k in range(n_k):
        to_core_own(k, own).start()

    def relay_x(k):
        with jax.named_scope("relay_x"):
            over_x(k, of_x).wait_recv()
        to_core_x(k, of_x).start()

    def relay_pair():
        with jax.named_scope("relay_p"):
            pair_over_x(of_x).wait_recv()
        pair_over_y(mine).start()
        pair_to_core(mine, 0, of_x).start()

    def relay_pair_y():
        with jax.named_scope("relay_py"):
            pair_over_y(other).wait_recv()
        pair_to_core(other, 1, of_x).start()

    with jax.named_scope("route_wait"):
        route_all.wait_recv()

    def route_row(j):
        return jnp.concatenate([route[b, j:j + 1, :] for b in range(4)], axis=1)

    row_code = (route_row(0), route_row(1))
    row_gate = (route_row(2), route_row(3))
    for e in range(2):
        slot = (lax.broadcasted_iota(jnp.int32, (cap, 4 * rows), 0) + (2 * ep + e) * cap).astype(F32)
        hit0, hit1 = row_code[0] == slot, row_code[1] == slot
        onehot[e] = jnp.where(hit0 | hit1, 1.0, 0.0).astype(BF16)
        g = jnp.where(hit0, row_gate[0], 0.0) + jnp.where(hit1, row_gate[1], 0.0)
        gate_col[e] = jnp.sum(g, axis=1, keepdims=True)

    def build_comb():
        k = lax.broadcasted_iota(jnp.int32, (rows, 4 * cap_local), 1)
        part = jnp.where(k >= 2 * cap_local, 1, 0)
        k = k - part * (2 * cap_local)
        sub = jnp.where(k >= cap_local, 1, 0)
        k = k - sub * cap_local
        dev_of = jnp.where(part == 0, ep, 2 * x + oc)
        with jax.named_scope("comb_mat"):
            for b in range(4):
                slot = ((2 * dev_of + sub) * cap + b * cap_local + k).astype(F32)
                back = jnp.concatenate([route[b]] * 16, axis=0).T
                hit = (back[:, 0:1] == slot) | (back[:, 1:2] == slot)
                one = jnp.where(hit, 1.0, 0.0).astype(BF16)
                comb[b] = jnp.concatenate([one, one, one], axis=1)

    def product(e, w, off, width, first, last):
        slot = w % GU_SLOTS
        depth = pl.ds(off, width)
        for lo in range(0, d_ff, NB):
            span = slice(lo, min(lo + NB, d_ff))
            part = [jnp.dot(xs[e, :, 0:width], wgu[slot, e, m, depth, span], preferred_element_type=F32)
                    for m in range(2)]
            if not first:
                part = [acc[e, m, :, span] + part[m] for m in range(2)]
            if last:
                act[e, :, span] = (jax.nn.silu(part[0]) * part[1]).astype(BF16)
            else:
                for m in range(2):
                    acc[e, m, :, span] = part[m]

    def gate_up(chunks, w, off, first=False, last=False):
        @pl.when(always)
        def _():
            with jax.named_scope("gu_dot"):
                for e in range(2):
                    for i, k in enumerate(chunks):
                        xs[e, :, i * PIECE:(i + 1) * PIECE] = jnp.dot(
                            onehot[e], tok[k], preferred_element_type=F32).astype(BF16)
                for e in range(2):
                    product(e, w, off, len(chunks) * PIECE, first, last)

    def have(*copies):
        with jax.named_scope("tok_wait"):
            for cp in copies:
                cp.wait_recv()

    def weights(w):
        with jax.named_scope("gu_wait"):
            gu_all(w).wait()

    relay_x(0)
    build_comb()
    relay_x(1)
    have(remote(tok.at[:, of_c], tok.at[:, of_c], s1_s, s1_r, dev_c), to_core_x(0, of_xc))
    weights(0)
    gate_up((0,), 0, 0, first=True)
    relay_pair()
    have(to_core_x(1, of_xc))
    gate_up((1,), 0, PIECE)
    for e in range(2):
        for m in range(2):
            gu_copy(GU_SLOTS, e, m).start(priority=1)
    relay_x(4)
    have(pair_to_core(mine, 0, of_xc))
    weights(1)
    gate_up((mine,), 1, pl.multiple_of(y * PIECE, PIECE))
    relay_x(5)
    have(to_core_x(4, of_xc))
    weights(2)
    gate_up((4,), 2, 0)
    relay_x(6)
    relay_pair_y()
    have(to_core_x(5, of_xc))
    gate_up((5,), 2, PIECE)
    relay_x(7)
    have(pair_to_core(other, 1, of_xc))
    gate_up((other,), 1, pl.multiple_of(oy * PIECE, PIECE))
    for u in range(WD_SLOTS):
        wd_copy(u).start(priority=1)
    have(to_core_x(6, of_xc), to_core_x(7, of_xc))
    weights(3)
    gate_up((6, 7), 3, 0, last=True)

    def dw(u):
        return remote(w_all.at[u, oc], w_recv.at[u], dw_s, dw_r.at[u], dev_c)

    def f1(u, pos):
        return remote(f1_send.at[u, pos], f1_recv.at[u, pos], f1_s, f1_r.at[u, pos],
                      dev_y if u in Y_FIRST else dev_x)

    def f2(u):
        return remote(f2_send.at[u], f2_recv.at[u], f2_s, f2_r.at[u], dev_x if u in Y_FIRST else dev_y)

    def out_cols(core, u):
        return pl.ds(pl.multiple_of(u * uw + core * hu, hu), hu)

    def to_other(u):
        return remote(fin.at[u], out_ref.at[:, out_cols(c, u)], fo_s.at[0], fo_r.at[c], dev_fin)

    def to_core(u):
        return remote(fin.at[u], out_ref.at[:, out_cols(c, u)], fo_s.at[1], fo_r.at[c], dev_c)

    def down(u):
        slot = u % WD_SLOTS
        with jax.named_scope("wd_wait"):
            wd_copy(u).wait()
        with jax.named_scope("wd_dot"):
            for e in range(2):
                out = jnp.dot(act[e], wdn[slot, e], preferred_element_type=F32) * gate_col[e]
                for core in range(2):
                    for b in range(4):
                        w_all[u, core, b, e * cap_local:(e + 1) * cap_local] = (
                            out[b * cap_local:(b + 1) * cap_local, core * hu:(core + 1) * hu])
        dw(u).start()
        if u + WD_SLOTS < N_U:
            wd_copy(u + WD_SLOTS).start(priority=1)

    def combine(u):
        with jax.named_scope("dw_wait"):
            dw(u).wait_recv()
        if u in Y_FIRST:
            keep1, send0 = 2 * ox + y, 2 * x + oy
        else:
            keep1, send0 = 2 * x + oy, 2 * ox + y
        with jax.named_scope("comb"):
            for dst, pos, b in ((f1_send, 1, 2 * ox + oy), (f1_send, 0, send0),
                                (f1_keep, 1, keep1), (f1_keep, 0, 2 * x + y)):
                s = jnp.concatenate([w_all[u, c, b], w_recv[u, b]], axis=0)
                hi = s.astype(BF16)
                rest = s - hi.astype(F32)
                mid = rest.astype(BF16)
                lo = (rest - mid.astype(F32)).astype(BF16)
                parts = jnp.concatenate([hi, mid, lo], axis=0)
                dst[u, pos] = jnp.dot(comb[b], parts, preferred_element_type=F32)
                if dst is f1_send and pos == 1 and u in AT_ONCE:
                    f1(u, 1).start()
    def second(u):
        with jax.named_scope("f1_wait"):
            f1(u, 1).wait_recv()
        f2_send[u] = f1_keep[u, 1] + f1_recv[u, 1]
        f2(u).start()

    def final(u):
        with jax.named_scope("f2_wait"):
            f1(u, 0).wait_recv()
            f2(u).wait_recv()
        fin[u] = (f1_keep[u, 0] + f1_recv[u, 0] + f2_recv[u]).astype(BF16)
        to_other(u).start()

        @pl.when(c == y)
        def _():
            out_ref[:, out_cols(c, u)] = fin[u]

        @pl.when(c != y)
        def _():
            to_core(u).start()

    steps = {"D": down, "C": combine, "S": lambda u: None if u in AT_ONCE else f1(u, 1).start(), "H": lambda u: f1(u, 0).start(),
             "A": second, "B": final}
    for step in ORDER:
        steps[step[0]](int(step[1:]))

    with jax.named_scope("end"):
        route_all.wait_send()
        remote(tok.at[:, own], tok.at[:, own], s1_s, s1_r, dev_c).wait_send()
        remote(tok.at[pl.ds(0, n_k - 1), own], tok.at[pl.ds(0, n_k - 1), own], xd_s, xd_r.at[0], dev_x).wait_send()
        pair_over_y(mine).wait_send()
        remote(tok.at[:, of_x], tok.at[:, of_x], c3_s, c3_r.at[0], dev_c).wait_send()
        remote(w_all.at[:, oc], w_recv, dw_s, dw_r.at[0], dev_c).wait_send()
        remote(f1_send, f1_recv, f1_s, f1_r.at[0, 0], dev_x).wait_send()
        remote(f2_send, f2_recv, f2_s, f2_r.at[0], dev_y).wait_send()
        remote(fin, fin, fo_s.at[0], fo_r.at[0], dev_fin).wait_send()

        @pl.when(c != y)
        def _():
            remote(fin, fin, fo_s.at[1], fo_r.at[0], dev_c).wait_send()
    with jax.named_scope("in_wait"):
        remote(fin, fin, fo_s.at[0], fo_r.at[oc], dev_fin).wait_recv()

        @pl.when(c != y)
        def _():
            remote(fin, fin, fo_s.at[0], fo_r.at[c], dev_fin).wait_recv()


def solution(mesh):
    group = mesh.shape['ep']
    row_spec = P(('dp', 'ep'), None)
    col_spec = P('ep', None, 'etp')
    in_specs = (row_spec, row_spec, row_spec, row_spec, col_spec, col_spec, P('ep', 'etp', None))

    def device_step(hidden, expert_ids, gate_wts, slot_pos, w_gate, w_up, w_down):
        rows, d_model = hidden.shape
        top_k = expert_ids.shape[1]
        local_experts = w_gate.shape[0]
        experts = local_experts * group
        cap_local = ((5 * top_k * rows) // (4 * experts) + 7) // 8 * 8
        cap = group * cap_local
        d_ff = w_gate.shape[2]
        hu = d_model // (2 * N_U)
        kw = d_model // N_W
        n_k = d_model // PIECE
        any_spec = pl.BlockSpec(memory_space=pl.ANY)
        vmem_spec = pl.BlockSpec(memory_space=pltpu.VMEM)
        dma = pltpu.SemaphoreType.DMA
        scratch = [
            pltpu.VMEM((top_k, rows), jnp.int32),
            pltpu.VMEM((top_k, rows), F32),
            pltpu.VMEM((top_k, rows), jnp.int32),
            pltpu.VMEM((d_model // PIECE, group * rows, PIECE), BF16),
            pltpu.VMEM((group, 8, 128), F32),
            pltpu.VMEM((2, cap, group * rows), BF16),
            pltpu.VMEM((group, rows, 12 * cap_local), BF16),
            pltpu.VMEM((2, cap, 1), F32),
            pltpu.VMEM((2, cap, 2 * PIECE), BF16),
            pltpu.VMEM((2, 2, cap, d_ff), F32),
            pltpu.VMEM((2, cap, d_ff), BF16),
            pltpu.VMEM((GU_SLOTS, 2, 2, kw, d_ff), BF16),
            pltpu.VMEM((WD_SLOTS, 2, d_ff, 2 * hu), BF16),
            pltpu.VMEM((N_U, 2, 4, 2 * cap_local, hu), F32),
            pltpu.VMEM((N_U, 4, 2 * cap_local, hu), F32),
            pltpu.VMEM((N_U, 2, rows, hu), F32),
            pltpu.VMEM((N_U, 2, rows, hu), F32),
            pltpu.VMEM((N_U, 2, rows, hu), F32),
            pltpu.VMEM((N_U, rows, hu), F32),
            pltpu.VMEM((N_U, rows, hu), F32),
            pltpu.VMEM((N_U, rows, hu), BF16),
            dma((3,)), dma, dma((GU_SLOTS,)), dma((WD_SLOTS,)), dma, dma, dma, dma,
            dma, dma((n_k,)), dma, dma, dma, dma((n_k,)),
            dma, dma((N_U,)), dma, dma((N_U, 2)), dma, dma((N_U,)), dma((2,)), dma((2,)),
        ]
        return pl.pallas_call(
            functools.partial(moe_kernel, rows, d_model, d_ff, cap_local),
            out_shape=pltpu.VMEM((rows, d_model), BF16),
            in_specs=[any_spec] * 7,
            out_specs=vmem_spec,
            scratch_shapes=scratch,
            compiler_params=pltpu.CompilerParams(collective_id=0, has_side_effects=True,
                                                 vmem_limit_bytes=66_400_000),
        )(hidden, expert_ids.T, gate_wts.T, slot_pos.T, w_gate, w_up, w_down)

    return jax.shard_map(device_step, mesh=mesh, in_specs=in_specs, out_specs=row_spec, check_vma=False)
```

```python
import functools
import jax
import jax.numpy as jnp
from jax import lax
from jax.sharding import PartitionSpec as P
from jax.experimental import pallas as pl
from jax.experimental.pallas import tpu as pltpu

MESH = pl.DeviceIdType.MESH
F32, BF16 = jnp.float32, jnp.bfloat16
N_W = 4
GU_SLOTS = 3
WD_SLOTS = 3
N_U = 8
NB = 256
PIECE = 256
PAIR = 2
Y_FIRST = (1, 3, 7)
AT_ONCE = (0, 1)
ORDER = (
    "D0", "D1", "D2", "C0", "S0", "C1", "S1", "D3", "H0", "C2", "H1", "D4",
    "S2", "C3", "S3", "D5", "D6", "H2", "C4", "A0", "D7", "C6", "S4", "H3",
    "S6", "C7", "A2", "A1", "S7", "A3", "H7", "C5", "S5", "B0", "A6", "A4",
    "A7", "H6", "B2", "B1", "H4", "A5", "H5", "B3", "B6", "B4", "B7", "B5",
)


def moe_kernel(rows, d_model, d_ff, cap_local,
               hid_hbm, ids_hbm, gates_hbm, pos_hbm, wg_hbm, wu_hbm, wd_hbm, out_ref,
               ids, gates, pos, tok, route, onehot, comb, gate_col, xs, acc, act, wgu, wdn,
               w_all, w_recv, f1_keep, f1_send, f1_recv, f2_send, f2_recv, fin,
               in_sem, hid_sem, gu_sem, pair_sem, wd_sem, rt_s, rt_r, s1_s, s1_r, xd_s, xd_r, yd_s, yd_r, c3_s, c3_r,
               dw_s, dw_r, f1_s, f1_r, f2_s, f2_r, fo_s, fo_r):
    cap = 4 * cap_local
    kw = d_model // N_W
    uw = d_model // N_U
    hu = uw // 2
    n_k = d_model // PIECE
    ep = lax.axis_index("ep")
    y = lax.axis_index("etp")
    c = lax.rem(ep, 2)
    x = ep // 2
    ox, oy, oc = 1 - x, 1 - y, 1 - c
    dev_c = {"ep": 2 * x + oc}
    dev_x = {"ep": 2 * ox + c}
    dev_xc = {"ep": 2 * ox + oc}
    dev_y = {"etp": oy}
    dev_yc = {"etp": oy, "ep": 2 * x + oc}
    dev_fin = {"etp": oy, "ep": 2 * x + y}
    always = ep >= 0

    def remote(src, dst, s, r, dev):
        return pltpu.make_async_remote_copy(src_ref=src, dst_ref=dst, send_sem=s, recv_sem=r,
                                            device_id=dev, device_id_type=MESH)

    def block(b):
        return pl.ds(pl.multiple_of(b * rows, rows), rows)

    own, of_c, of_x, of_xc = block(ep), block(2 * x + oc), block(2 * ox + c), block(2 * ox + oc)

    barrier = pltpu.get_barrier_semaphore()
    for dev in (dev_c, dev_x, dev_xc, dev_y, dev_yc):
        pl.semaphore_signal(barrier, inc=1, device_id=dev, device_id_type=MESH)

    def hid_copy(i):
        return pltpu.make_async_copy(hid_hbm.at[:, i * PIECE:(i + 1) * PIECE], tok.at[i, own], hid_sem)

    hid_all = pltpu.make_async_copy(tok.at[:, own], tok.at[:, own], hid_sem)

    def gu_copy(w, e, m):
        slot = w % GU_SLOTS
        src = (wg_hbm, wu_hbm)[m]
        return pltpu.make_async_copy(src.at[e, pl.ds(w * kw, kw)], wgu.at[slot, e, m], gu_sem.at[slot])

    def gu_all(w):
        slot = w % GU_SLOTS
        return pltpu.make_async_copy(wgu.at[slot], wgu.at[slot], gu_sem.at[slot])

    def wd_copy(u):
        slot = u % WD_SLOTS
        return pltpu.make_async_copy(wd_hbm.at[:, :, pl.ds(u * uw, uw)], wdn.at[slot], wd_sem.at[slot])

    route_in = [pltpu.make_async_copy(src, dst, in_sem.at[i])
                for i, (src, dst) in enumerate(((ids_hbm, ids), (gates_hbm, gates), (pos_hbm, pos)))]
    for cp in route_in:
        cp.start()
    for i in range(n_k):
        hid_copy(i).start()
    pair_w = PAIR * PIECE // kw

    def pair_rows(i):
        return pl.ds(pl.multiple_of((y if i == 0 else oy) * PIECE, PIECE), PIECE)

    def pair_copy(i, e, m):
        src = (wg_hbm, wu_hbm)[m]
        rows_in = pl.ds(pl.multiple_of(pair_w * kw + (y if i == 0 else oy) * PIECE, PIECE), PIECE)
        return pltpu.make_async_copy(src.at[e, rows_in], wgu.at[pair_w, e, m, pair_rows(i)], pair_sem.at[i])

    def pair_all(i):
        half = wgu.at[pair_w, :, :, pair_rows(i)]
        return pltpu.make_async_copy(half, half, pair_sem.at[i])

    for load in ((lambda e, m: gu_copy(0, e, m)), (lambda e, m: pair_copy(0, e, m)),
                 (lambda e, m: gu_copy(2, e, m)), (lambda e, m: pair_copy(1, e, m))):
        for e in range(2):
            for m in range(2):
                load(e, m).start(priority=1)

    for cp in route_in:
        cp.wait()
    code = jnp.where(pos[...] >= 0, ids[...] * cap + pos[...], -1).astype(F32)
    route[ep] = jnp.concatenate([code, gates[...], jnp.zeros((4, rows), F32)], axis=0)
    with jax.named_scope("hid_wait"):
        hid_all.wait()
    with jax.named_scope("barrier"):
        pl.semaphore_wait(barrier, 5)

    def route_copy(i, b):
        return remote(route.at[b], route.at[b], rt_s, rt_r, route_devs[i])

    route_all = remote(route.at[pl.ds(0, 3)], route.at[pl.ds(0, 3)], rt_s, rt_r, dev_c)

    def to_core_own(k, blk):
        return remote(tok.at[k, blk], tok.at[k, blk], s1_s, s1_r, dev_c)

    def over_x(k, blk):
        return remote(tok.at[k, blk], tok.at[k, blk], xd_s, xd_r.at[k], dev_x)

    def to_core_x(k, blk):
        return remote(tok.at[k, blk], tok.at[k, blk], c3_s, c3_r.at[k], dev_c)

    route_devs = (dev_c, dev_x, dev_xc)
    for i in range(3):
        route_copy(i, ep).start()
    mine, other = PAIR + y, PAIR + oy

    def pair_over_x(blk):
        return remote(tok.at[mine, blk], tok.at[mine, blk], xd_s, xd_r.at[PAIR], dev_x)

    def pair_over_y(k):
        return remote(tok.at[k, of_x], tok.at[k, of_x], yd_s, yd_r, dev_y)

    def pair_to_core(k, i, blk):
        return remote(tok.at[k, blk], tok.at[k, blk], c3_s, c3_r.at[PAIR + i], dev_c)

    for k in range(n_k):
        if k == PAIR:
            pair_over_x(own).start()
        elif k != PAIR + 1:
            over_x(k, own).start()
    for k in range(n_k):
        to_core_own(k, own).start()

    def relay_x(k):
        with jax.named_scope("relay_x"):
            over_x(k, of_x).wait_recv()
        to_core_x(k, of_x).start()

    def relay_pair():
        with jax.named_scope("relay_p"):
            pair_over_x(of_x).wait_recv()
        pair_over_y(mine).start()
        pair_to_core(mine, 0, of_x).start()

    def relay_pair_y():
        with jax.named_scope("relay_py"):
            pair_over_y(other).wait_recv()
        pair_to_core(other, 1, of_x).start()

    with jax.named_scope("route_wait"):
        route_all.wait_recv()

    def route_row(j):
        return jnp.concatenate([route[b, j:j + 1, :] for b in range(4)], axis=1)

    row_code = (route_row(0), route_row(1))
    row_gate = (route_row(2), route_row(3))
    for e in range(2):
        slot = (lax.broadcasted_iota(jnp.int32, (cap, 4 * rows), 0) + (2 * ep + e) * cap).astype(F32)
        hit0, hit1 = row_code[0] == slot, row_code[1] == slot
        onehot[e] = jnp.where(hit0 | hit1, 1.0, 0.0).astype(BF16)
        g = jnp.where(hit0, row_gate[0], 0.0) + jnp.where(hit1, row_gate[1], 0.0)
        gate_col[e] = jnp.sum(g, axis=1, keepdims=True)

    def build_comb():
        k = lax.broadcasted_iota(jnp.int32, (rows, 4 * cap_local), 1)
        part = jnp.where(k >= 2 * cap_local, 1, 0)
        k = k - part * (2 * cap_local)
        sub = jnp.where(k >= cap_local, 1, 0)
        k = k - sub * cap_local
        dev_of = jnp.where(part == 0, ep, 2 * x + oc)
        with jax.named_scope("comb_mat"):
            for b in range(4):
                slot = ((2 * dev_of + sub) * cap + b * cap_local + k).astype(F32)
                back = jnp.concatenate([route[b]] * 16, axis=0).T
                hit = (back[:, 0:1] == slot) | (back[:, 1:2] == slot)
                one = jnp.where(hit, 1.0, 0.0).astype(BF16)
                comb[b] = jnp.concatenate([one, one, one], axis=1)

    def product(e, w, off, width, first, last):
        slot = w % GU_SLOTS
        depth = pl.ds(off, width)
        for lo in range(0, d_ff, NB):
            span = slice(lo, min(lo + NB, d_ff))
            part = [jnp.dot(xs[e, :, 0:width], wgu[slot, e, m, depth, span], preferred_element_type=F32)
                    for m in range(2)]
            if not first:
                part = [acc[e, m, :, span] + part[m] for m in range(2)]
            if last:
                act[e, :, span] = (jax.nn.silu(part[0]) * part[1]).astype(BF16)
            else:
                for m in range(2):
                    acc[e, m, :, span] = part[m]

    def gate_up(chunks, w, off, first=False, last=False):
        @pl.when(always)
        def _():
            with jax.named_scope("gu_dot"):
                for e in range(2):
                    for i, k in enumerate(chunks):
                        xs[e, :, i * PIECE:(i + 1) * PIECE] = jnp.dot(
                            onehot[e], tok[k], preferred_element_type=F32).astype(BF16)
                for e in range(2):
                    product(e, w, off, len(chunks) * PIECE, first, last)

    def have(*copies):
        with jax.named_scope("tok_wait"):
            for cp in copies:
                cp.wait_recv()

    def weights(w):
        with jax.named_scope("gu_wait"):
            gu_all(w).wait()

    relay_x(0)
    build_comb()
    relay_x(1)
    have(remote(tok.at[:, of_c], tok.at[:, of_c], s1_s, s1_r, dev_c), to_core_x(0, of_xc))
    weights(0)
    gate_up((0,), 0, 0, first=True)
    relay_pair()
    have(to_core_x(1, of_xc))
    gate_up((1,), 0, PIECE)
    for e in range(2):
        for m in range(2):
            gu_copy(GU_SLOTS, e, m).start(priority=1)
    relay_x(4)
    have(pair_to_core(mine, 0, of_xc))
    with jax.named_scope("gu_wait"):
        pair_all(0).wait()
    gate_up((mine,), 1, pl.multiple_of(y * PIECE, PIECE))
    relay_x(5)
    have(to_core_x(4, of_xc))
    weights(2)
    gate_up((4,), 2, 0)
    relay_x(6)
    relay_pair_y()
    have(to_core_x(5, of_xc))
    gate_up((5,), 2, PIECE)
    relay_x(7)
    have(pair_to_core(other, 1, of_xc))
    with jax.named_scope("gu_wait"):
        pair_all(1).wait()
    gate_up((other,), 1, pl.multiple_of(oy * PIECE, PIECE))
    for u in range(WD_SLOTS):
        wd_copy(u).start(priority=1)
    have(to_core_x(6, of_xc), to_core_x(7, of_xc))
    weights(3)
    gate_up((6, 7), 3, 0, last=True)

    def dw(u):
        return remote(w_all.at[u, oc], w_recv.at[u], dw_s, dw_r.at[u], dev_c)

    def f1(u, pos):
        return remote(f1_send.at[u, pos], f1_recv.at[u, pos], f1_s, f1_r.at[u, pos],
                      dev_y if u in Y_FIRST else dev_x)

    def f2(u):
        return remote(f2_send.at[u], f2_recv.at[u], f2_s, f2_r.at[u], dev_x if u in Y_FIRST else dev_y)

    def out_cols(core, u):
        return pl.ds(pl.multiple_of(u * uw + core * hu, hu), hu)

    def to_other(u):
        return remote(fin.at[u], out_ref.at[:, out_cols(c, u)], fo_s.at[0], fo_r.at[c], dev_fin)

    def to_core(u):
        return remote(fin.at[u], out_ref.at[:, out_cols(c, u)], fo_s.at[1], fo_r.at[c], dev_c)

    def down(u):
        slot = u % WD_SLOTS
        with jax.named_scope("wd_wait"):
            wd_copy(u).wait()
        with jax.named_scope("wd_dot"):
            for e in range(2):
                out = jnp.dot(act[e], wdn[slot, e], preferred_element_type=F32) * gate_col[e]
                for core in range(2):
                    for b in range(4):
                        w_all[u, core, b, e * cap_local:(e + 1) * cap_local] = (
                            out[b * cap_local:(b + 1) * cap_local, core * hu:(core + 1) * hu])
        dw(u).start()
        if u + WD_SLOTS < N_U:
            wd_copy(u + WD_SLOTS).start(priority=1)

    def combine(u):
        with jax.named_scope("dw_wait"):
            dw(u).wait_recv()
        if u in Y_FIRST:
            keep1, send0 = 2 * ox + y, 2 * x + oy
        else:
            keep1, send0 = 2 * x + oy, 2 * ox + y
        with jax.named_scope("comb"):
            for dst, pos, b in ((f1_send, 1, 2 * ox + oy), (f1_send, 0, send0),
                                (f1_keep, 1, keep1), (f1_keep, 0, 2 * x + y)):
                s = jnp.concatenate([w_all[u, c, b], w_recv[u, b]], axis=0)
                hi = s.astype(BF16)
                rest = s - hi.astype(F32)
                mid = rest.astype(BF16)
                lo = (rest - mid.astype(F32)).astype(BF16)
                parts = jnp.concatenate([hi, mid, lo], axis=0)
                dst[u, pos] = jnp.dot(comb[b], parts, preferred_element_type=F32)
                if dst is f1_send and pos == 1 and u in AT_ONCE:
                    f1(u, 1).start()
    def second(u):
        with jax.named_scope("f1_wait"):
            f1(u, 1).wait_recv()
        f2_send[u] = f1_keep[u, 1] + f1_recv[u, 1]
        f2(u).start()

    def final(u):
        with jax.named_scope("f2_wait"):
            f1(u, 0).wait_recv()
            f2(u).wait_recv()
        fin[u] = (f1_keep[u, 0] + f1_recv[u, 0] + f2_recv[u]).astype(BF16)
        to_other(u).start()

        @pl.when(c == y)
        def _():
            out_ref[:, out_cols(c, u)] = fin[u]

        @pl.when(c != y)
        def _():
            to_core(u).start()

    steps = {"D": down, "C": combine, "S": lambda u: None if u in AT_ONCE else f1(u, 1).start(), "H": lambda u: f1(u, 0).start(),
             "A": second, "B": final}
    for step in ORDER:
        steps[step[0]](int(step[1:]))

    with jax.named_scope("end"):
        route_all.wait_send()
        remote(tok.at[:, own], tok.at[:, own], s1_s, s1_r, dev_c).wait_send()
        remote(tok.at[pl.ds(0, n_k - 1), own], tok.at[pl.ds(0, n_k - 1), own], xd_s, xd_r.at[0], dev_x).wait_send()
        pair_over_y(mine).wait_send()
        remote(tok.at[:, of_x], tok.at[:, of_x], c3_s, c3_r.at[0], dev_c).wait_send()
        remote(w_all.at[:, oc], w_recv, dw_s, dw_r.at[0], dev_c).wait_send()
        remote(f1_send, f1_recv, f1_s, f1_r.at[0, 0], dev_x).wait_send()
        remote(f2_send, f2_recv, f2_s, f2_r.at[0], dev_y).wait_send()
        remote(fin, fin, fo_s.at[0], fo_r.at[0], dev_fin).wait_send()

        @pl.when(c != y)
        def _():
            remote(fin, fin, fo_s.at[1], fo_r.at[0], dev_c).wait_send()
    with jax.named_scope("in_wait"):
        remote(fin, fin, fo_s.at[0], fo_r.at[oc], dev_fin).wait_recv()

        @pl.when(c != y)
        def _():
            remote(fin, fin, fo_s.at[0], fo_r.at[c], dev_fin).wait_recv()


def solution(mesh):
    group = mesh.shape['ep']
    row_spec = P(('dp', 'ep'), None)
    col_spec = P('ep', None, 'etp')
    in_specs = (row_spec, row_spec, row_spec, row_spec, col_spec, col_spec, P('ep', 'etp', None))

    def device_step(hidden, expert_ids, gate_wts, slot_pos, w_gate, w_up, w_down):
        rows, d_model = hidden.shape
        top_k = expert_ids.shape[1]
        local_experts = w_gate.shape[0]
        experts = local_experts * group
        cap_local = ((5 * top_k * rows) // (4 * experts) + 7) // 8 * 8
        cap = group * cap_local
        d_ff = w_gate.shape[2]
        hu = d_model // (2 * N_U)
        kw = d_model // N_W
        n_k = d_model // PIECE
        any_spec = pl.BlockSpec(memory_space=pl.ANY)
        vmem_spec = pl.BlockSpec(memory_space=pltpu.VMEM)
        dma = pltpu.SemaphoreType.DMA
        scratch = [
            pltpu.VMEM((top_k, rows), jnp.int32),
            pltpu.VMEM((top_k, rows), F32),
            pltpu.VMEM((top_k, rows), jnp.int32),
            pltpu.VMEM((d_model // PIECE, group * rows, PIECE), BF16),
            pltpu.VMEM((group, 8, 128), F32),
            pltpu.VMEM((2, cap, group * rows), BF16),
            pltpu.VMEM((group, rows, 12 * cap_local), BF16),
            pltpu.VMEM((2, cap, 1), F32),
            pltpu.VMEM((2, cap, 2 * PIECE), BF16),
            pltpu.VMEM((2, 2, cap, d_ff), F32),
            pltpu.VMEM((2, cap, d_ff), BF16),
            pltpu.VMEM((GU_SLOTS, 2, 2, kw, d_ff), BF16),
            pltpu.VMEM((WD_SLOTS, 2, d_ff, 2 * hu), BF16),
            pltpu.VMEM((N_U, 2, 4, 2 * cap_local, hu), F32),
            pltpu.VMEM((N_U, 4, 2 * cap_local, hu), F32),
            pltpu.VMEM((N_U, 2, rows, hu), F32),
            pltpu.VMEM((N_U, 2, rows, hu), F32),
            pltpu.VMEM((N_U, 2, rows, hu), F32),
            pltpu.VMEM((N_U, rows, hu), F32),
            pltpu.VMEM((N_U, rows, hu), F32),
            pltpu.VMEM((N_U, rows, hu), BF16),
            dma((3,)), dma, dma((GU_SLOTS,)), dma((2,)), dma((WD_SLOTS,)), dma, dma, dma, dma,
            dma, dma((n_k,)), dma, dma, dma, dma((n_k,)),
            dma, dma((N_U,)), dma, dma((N_U, 2)), dma, dma((N_U,)), dma((2,)), dma((2,)),
        ]
        return pl.pallas_call(
            functools.partial(moe_kernel, rows, d_model, d_ff, cap_local),
            out_shape=pltpu.VMEM((rows, d_model), BF16),
            in_specs=[any_spec] * 7,
            out_specs=vmem_spec,
            scratch_shapes=scratch,
            compiler_params=pltpu.CompilerParams(collective_id=0, has_side_effects=True,
                                                 vmem_limit_bytes=66_400_000),
        )(hidden, expert_ids.T, gate_wts.T, slot_pos.T, w_gate, w_up, w_down)

    return jax.shard_map(device_step, mesh=mesh, in_specs=in_specs, out_specs=row_spec, check_vma=False)
```

```python
import functools
import jax
import jax.numpy as jnp
from jax import lax
from jax.sharding import PartitionSpec as P
from jax.experimental import pallas as pl
from jax.experimental.pallas import tpu as pltpu

MESH = pl.DeviceIdType.MESH
F32, BF16 = jnp.float32, jnp.bfloat16
N_W = 4
GU_SLOTS = 3
WD_SLOTS = 3
N_U = 8
NB = 256
PIECE = 256
PAIR = 2
Y_FIRST = (1, 3, 7)
AT_ONCE = (0, 1)
ORDER = (
    "D0", "D1", "D2", "C0", "C1", "R0", "H0", "R1", "D3", "C2", "H1", "D4",
    "S2", "C3", "S3", "D5", "D6", "H2", "C4", "A0", "D7", "C6", "S4", "H3",
    "S6", "C7", "A2", "A1", "S7", "A3", "H7", "C5", "S5", "B0", "A6", "A4",
    "A7", "H6", "B2", "B1", "H4", "A5", "H5", "B3", "B6", "B4", "B7", "B5",
)


def moe_kernel(rows, d_model, d_ff, cap_local,
               hid_hbm, ids_hbm, gates_hbm, pos_hbm, wg_hbm, wu_hbm, wd_hbm, out_ref,
               ids, gates, pos, tok, route, onehot, comb, gate_col, xs, acc, act, wgu, wdn,
               w_all, w_recv, f1_keep, f1_send, f1_recv, f2_send, f2_recv, fin,
               in_sem, hid_sem, gu_sem, pair_sem, wd_sem, rt_s, rt_r, s1_s, s1_r, xd_s, xd_r, yd_s, yd_r, c3_s, c3_r,
               dw_s, dw_r, f1_s, f1_r, f2_s, f2_r, fo_s, fo_r):
    cap = 4 * cap_local
    kw = d_model // N_W
    uw = d_model // N_U
    hu = uw // 2
    n_k = d_model // PIECE
    ep = lax.axis_index("ep")
    y = lax.axis_index("etp")
    c = lax.rem(ep, 2)
    x = ep // 2
    ox, oy, oc = 1 - x, 1 - y, 1 - c
    dev_c = {"ep": 2 * x + oc}
    dev_x = {"ep": 2 * ox + c}
    dev_xc = {"ep": 2 * ox + oc}
    dev_y = {"etp": oy}
    dev_yc = {"etp": oy, "ep": 2 * x + oc}
    dev_fin = {"etp": oy, "ep": 2 * x + y}
    always = ep >= 0

    def remote(src, dst, s, r, dev):
        return pltpu.make_async_remote_copy(src_ref=src, dst_ref=dst, send_sem=s, recv_sem=r,
                                            device_id=dev, device_id_type=MESH)

    def block(b):
        return pl.ds(pl.multiple_of(b * rows, rows), rows)

    own, of_c, of_x, of_xc = block(ep), block(2 * x + oc), block(2 * ox + c), block(2 * ox + oc)

    barrier = pltpu.get_barrier_semaphore()
    for dev in (dev_c, dev_x, dev_xc, dev_y, dev_yc):
        pl.semaphore_signal(barrier, inc=1, device_id=dev, device_id_type=MESH)

    def hid_copy(i):
        return pltpu.make_async_copy(hid_hbm.at[:, i * PIECE:(i + 1) * PIECE], tok.at[i, own], hid_sem)

    hid_all = pltpu.make_async_copy(tok.at[:, own], tok.at[:, own], hid_sem)

    def gu_copy(w, e, m):
        slot = w % GU_SLOTS
        src = (wg_hbm, wu_hbm)[m]
        return pltpu.make_async_copy(src.at[e, pl.ds(w * kw, kw)], wgu.at[slot, e, m], gu_sem.at[slot])

    def gu_all(w):
        slot = w % GU_SLOTS
        return pltpu.make_async_copy(wgu.at[slot], wgu.at[slot], gu_sem.at[slot])

    def wd_copy(u):
        slot = u % WD_SLOTS
        return pltpu.make_async_copy(wd_hbm.at[:, :, pl.ds(u * uw, uw)], wdn.at[slot], wd_sem.at[slot])

    route_in = [pltpu.make_async_copy(src, dst, in_sem.at[i])
                for i, (src, dst) in enumerate(((ids_hbm, ids), (gates_hbm, gates), (pos_hbm, pos)))]
    for cp in route_in:
        cp.start()
    for i in range(n_k):
        hid_copy(i).start()
    pair_w = PAIR * PIECE // kw

    def pair_rows(i):
        return pl.ds(pl.multiple_of((y if i == 0 else oy) * PIECE, PIECE), PIECE)

    def pair_copy(i, e, m):
        src = (wg_hbm, wu_hbm)[m]
        rows_in = pl.ds(pl.multiple_of(pair_w * kw + (y if i == 0 else oy) * PIECE, PIECE), PIECE)
        return pltpu.make_async_copy(src.at[e, rows_in], wgu.at[pair_w, e, m, pair_rows(i)], pair_sem.at[i])

    def pair_all(i):
        half = wgu.at[pair_w, :, :, pair_rows(i)]
        return pltpu.make_async_copy(half, half, pair_sem.at[i])

    for load in ((lambda e, m: gu_copy(0, e, m)), (lambda e, m: pair_copy(0, e, m)),
                 (lambda e, m: gu_copy(2, e, m)), (lambda e, m: pair_copy(1, e, m))):
        for e in range(2):
            for m in range(2):
                load(e, m).start(priority=1)

    for cp in route_in:
        cp.wait()
    code = jnp.where(pos[...] >= 0, ids[...] * cap + pos[...], -1).astype(F32)
    route[ep] = jnp.concatenate([code, gates[...], jnp.zeros((4, rows), F32)], axis=0)
    with jax.named_scope("hid_wait"):
        hid_all.wait()
    with jax.named_scope("barrier"):
        pl.semaphore_wait(barrier, 5)

    def route_copy(i, b):
        return remote(route.at[b], route.at[b], rt_s, rt_r, route_devs[i])

    route_all = remote(route.at[pl.ds(0, 3)], route.at[pl.ds(0, 3)], rt_s, rt_r, dev_c)

    def to_core_own(k, blk):
        return remote(tok.at[k, blk], tok.at[k, blk], s1_s, s1_r, dev_c)

    def over_x(k, blk):
        return remote(tok.at[k, blk], tok.at[k, blk], xd_s, xd_r.at[k], dev_x)

    def to_core_x(k, blk):
        return remote(tok.at[k, blk], tok.at[k, blk], c3_s, c3_r.at[k], dev_c)

    route_devs = (dev_c, dev_x, dev_xc)
    for i in range(3):
        route_copy(i, ep).start()
    mine, other = PAIR + y, PAIR + oy

    def pair_over_x(blk):
        return remote(tok.at[mine, blk], tok.at[mine, blk], xd_s, xd_r.at[PAIR], dev_x)

    def pair_over_y(k):
        return remote(tok.at[k, of_x], tok.at[k, of_x], yd_s, yd_r, dev_y)

    def pair_to_core(k, i, blk):
        return remote(tok.at[k, blk], tok.at[k, blk], c3_s, c3_r.at[PAIR + i], dev_c)

    for k in range(n_k):
        if k == PAIR:
            pair_over_x(own).start()
        elif k != PAIR + 1:
            over_x(k, own).start()
    for k in range(n_k):
        to_core_own(k, own).start()

    def relay_x(k):
        with jax.named_scope("relay_x"):
            over_x(k, of_x).wait_recv()
        to_core_x(k, of_x).start()

    def relay_pair():
        with jax.named_scope("relay_p"):
            pair_over_x(of_x).wait_recv()
        pair_over_y(mine).start()
        pair_to_core(mine, 0, of_x).start()

    def relay_pair_y():
        with jax.named_scope("relay_py"):
            pair_over_y(other).wait_recv()
        pair_to_core(other, 1, of_x).start()

    with jax.named_scope("route_wait"):
        route_all.wait_recv()

    def route_row(j):
        return jnp.concatenate([route[b, j:j + 1, :] for b in range(4)], axis=1)

    row_code = (route_row(0), route_row(1))
    row_gate = (route_row(2), route_row(3))
    for e in range(2):
        slot = (lax.broadcasted_iota(jnp.int32, (cap, 4 * rows), 0) + (2 * ep + e) * cap).astype(F32)
        hit0, hit1 = row_code[0] == slot, row_code[1] == slot
        onehot[e] = jnp.where(hit0 | hit1, 1.0, 0.0).astype(BF16)
        g = jnp.where(hit0, row_gate[0], 0.0) + jnp.where(hit1, row_gate[1], 0.0)
        gate_col[e] = jnp.sum(g, axis=1, keepdims=True)

    def build_comb():
        k = lax.broadcasted_iota(jnp.int32, (rows, 4 * cap_local), 1)
        part = jnp.where(k >= 2 * cap_local, 1, 0)
        k = k - part * (2 * cap_local)
        sub = jnp.where(k >= cap_local, 1, 0)
        k = k - sub * cap_local
        dev_of = jnp.where(part == 0, ep, 2 * x + oc)
        with jax.named_scope("comb_mat"):
            for b in range(4):
                slot = ((2 * dev_of + sub) * cap + b * cap_local + k).astype(F32)
                back = jnp.concatenate([route[b]] * 16, axis=0).T
                hit = (back[:, 0:1] == slot) | (back[:, 1:2] == slot)
                one = jnp.where(hit, 1.0, 0.0).astype(BF16)
                comb[b] = jnp.concatenate([one, one, one], axis=1)

    def product(e, w, off, width, first, last):
        slot = w % GU_SLOTS
        depth = pl.ds(off, width)
        for lo in range(0, d_ff, NB):
            span = slice(lo, min(lo + NB, d_ff))
            part = [jnp.dot(xs[e, :, 0:width], wgu[slot, e, m, depth, span], preferred_element_type=F32)
                    for m in range(2)]
            if not first:
                part = [acc[e, m, :, span] + part[m] for m in range(2)]
            if last:
                act[e, :, span] = (jax.nn.silu(part[0]) * part[1]).astype(BF16)
            else:
                for m in range(2):
                    acc[e, m, :, span] = part[m]

    def gate_up(chunks, w, off, first=False, last=False):
        @pl.when(always)
        def _():
            with jax.named_scope("gu_dot"):
                for e in range(2):
                    for i, k in enumerate(chunks):
                        xs[e, :, i * PIECE:(i + 1) * PIECE] = jnp.dot(
                            onehot[e], tok[k], preferred_element_type=F32).astype(BF16)
                for e in range(2):
                    product(e, w, off, len(chunks) * PIECE, first, last)

    def have(*copies):
        with jax.named_scope("tok_wait"):
            for cp in copies:
                cp.wait_recv()

    def weights(w):
        with jax.named_scope("gu_wait"):
            gu_all(w).wait()

    relay_x(0)
    build_comb()
    relay_x(1)
    have(remote(tok.at[:, of_c], tok.at[:, of_c], s1_s, s1_r, dev_c), to_core_x(0, of_xc))
    weights(0)
    gate_up((0,), 0, 0, first=True)
    relay_pair()
    have(to_core_x(1, of_xc))
    gate_up((1,), 0, PIECE)
    for e in range(2):
        for m in range(2):
            gu_copy(GU_SLOTS, e, m).start(priority=1)
    relay_x(4)
    have(pair_to_core(mine, 0, of_xc))
    with jax.named_scope("gu_wait"):
        pair_all(0).wait()
    gate_up((mine,), 1, pl.multiple_of(y * PIECE, PIECE))
    relay_x(5)
    have(to_core_x(4, of_xc))
    weights(2)
    gate_up((4,), 2, 0)
    relay_x(6)
    relay_pair_y()
    have(to_core_x(5, of_xc))
    gate_up((5,), 2, PIECE)
    relay_x(7)
    have(pair_to_core(other, 1, of_xc))
    with jax.named_scope("gu_wait"):
        pair_all(1).wait()
    gate_up((other,), 1, pl.multiple_of(oy * PIECE, PIECE))
    for u in range(WD_SLOTS):
        wd_copy(u).start(priority=1)
    have(to_core_x(6, of_xc), to_core_x(7, of_xc))
    weights(3)
    gate_up((6, 7), 3, 0, last=True)

    def dw(u):
        return remote(w_all.at[u, oc], w_recv.at[u], dw_s, dw_r.at[u], dev_c)

    def f1(u, pos):
        return remote(f1_send.at[u, pos], f1_recv.at[u, pos], f1_s, f1_r.at[u, pos],
                      dev_y if u in Y_FIRST else dev_x)

    def f2(u):
        return remote(f2_send.at[u], f2_recv.at[u], f2_s, f2_r.at[u], dev_x if u in Y_FIRST else dev_y)

    def out_cols(core, u):
        return pl.ds(pl.multiple_of(u * uw + core * hu, hu), hu)

    def to_other(u):
        return remote(fin.at[u], out_ref.at[:, out_cols(c, u)], fo_s.at[0], fo_r.at[c], dev_fin)

    def to_core(u):
        return remote(fin.at[u], out_ref.at[:, out_cols(c, u)], fo_s.at[1], fo_r.at[c], dev_c)

    def down(u):
        slot = u % WD_SLOTS
        with jax.named_scope("wd_wait"):
            wd_copy(u).wait()
        with jax.named_scope("wd_dot"):
            for e in range(2):
                out = jnp.dot(act[e], wdn[slot, e], preferred_element_type=F32) * gate_col[e]
                for core in range(2):
                    for b in range(4):
                        w_all[u, core, b, e * cap_local:(e + 1) * cap_local] = (
                            out[b * cap_local:(b + 1) * cap_local, core * hu:(core + 1) * hu])
        dw(u).start()
        if u + WD_SLOTS < N_U:
            wd_copy(u + WD_SLOTS).start(priority=1)

    def combine(u):
        with jax.named_scope("dw_wait"):
            dw(u).wait_recv()
        blocks(u, slice(0, 1 if u in AT_ONCE else 4))
        if u in AT_ONCE:
            f1(u, 1).start()

    def rest(u):
        blocks(u, slice(1, 4))

    def blocks(u, which):
        if u in Y_FIRST:
            keep1, send0 = 2 * ox + y, 2 * x + oy
        else:
            keep1, send0 = 2 * x + oy, 2 * ox + y
        with jax.named_scope("comb"):
            for dst, pos, b in ((f1_send, 1, 2 * ox + oy), (f1_send, 0, send0),
                                (f1_keep, 1, keep1), (f1_keep, 0, 2 * x + y))[which]:
                s = jnp.concatenate([w_all[u, c, b], w_recv[u, b]], axis=0)
                hi = s.astype(BF16)
                rest = s - hi.astype(F32)
                mid = rest.astype(BF16)
                lo = (rest - mid.astype(F32)).astype(BF16)
                parts = jnp.concatenate([hi, mid, lo], axis=0)
                dst[u, pos] = jnp.dot(comb[b], parts, preferred_element_type=F32)
    def second(u):
        with jax.named_scope("f1_wait"):
            f1(u, 1).wait_recv()
        f2_send[u] = f1_keep[u, 1] + f1_recv[u, 1]
        f2(u).start()

    def final(u):
        with jax.named_scope("f2_wait"):
            f1(u, 0).wait_recv()
            f2(u).wait_recv()
        fin[u] = (f1_keep[u, 0] + f1_recv[u, 0] + f2_recv[u]).astype(BF16)
        to_other(u).start()

        @pl.when(c == y)
        def _():
            out_ref[:, out_cols(c, u)] = fin[u]

        @pl.when(c != y)
        def _():
            to_core(u).start()

    steps = {"D": down, "C": combine, "R": rest, "S": lambda u: f1(u, 1).start(), "H": lambda u: f1(u, 0).start(),
             "A": second, "B": final}
    for step in ORDER:
        steps[step[0]](int(step[1:]))

    with jax.named_scope("end"):
        route_all.wait_send()
        remote(tok.at[:, own], tok.at[:, own], s1_s, s1_r, dev_c).wait_send()
        remote(tok.at[pl.ds(0, n_k - 1), own], tok.at[pl.ds(0, n_k - 1), own], xd_s, xd_r.at[0], dev_x).wait_send()
        pair_over_y(mine).wait_send()
        remote(tok.at[:, of_x], tok.at[:, of_x], c3_s, c3_r.at[0], dev_c).wait_send()
        remote(w_all.at[:, oc], w_recv, dw_s, dw_r.at[0], dev_c).wait_send()
        remote(f1_send, f1_recv, f1_s, f1_r.at[0, 0], dev_x).wait_send()
        remote(f2_send, f2_recv, f2_s, f2_r.at[0], dev_y).wait_send()
        remote(fin, fin, fo_s.at[0], fo_r.at[0], dev_fin).wait_send()

        @pl.when(c != y)
        def _():
            remote(fin, fin, fo_s.at[1], fo_r.at[0], dev_c).wait_send()
    with jax.named_scope("in_wait"):
        remote(fin, fin, fo_s.at[0], fo_r.at[oc], dev_fin).wait_recv()

        @pl.when(c != y)
        def _():
            remote(fin, fin, fo_s.at[0], fo_r.at[c], dev_fin).wait_recv()


def solution(mesh):
    group = mesh.shape['ep']
    row_spec = P(('dp', 'ep'), None)
    col_spec = P('ep', None, 'etp')
    in_specs = (row_spec, row_spec, row_spec, row_spec, col_spec, col_spec, P('ep', 'etp', None))

    def device_step(hidden, expert_ids, gate_wts, slot_pos, w_gate, w_up, w_down):
        rows, d_model = hidden.shape
        top_k = expert_ids.shape[1]
        local_experts = w_gate.shape[0]
        experts = local_experts * group
        cap_local = ((5 * top_k * rows) // (4 * experts) + 7) // 8 * 8
        cap = group * cap_local
        d_ff = w_gate.shape[2]
        hu = d_model // (2 * N_U)
        kw = d_model // N_W
        n_k = d_model // PIECE
        any_spec = pl.BlockSpec(memory_space=pl.ANY)
        vmem_spec = pl.BlockSpec(memory_space=pltpu.VMEM)
        dma = pltpu.SemaphoreType.DMA
        scratch = [
            pltpu.VMEM((top_k, rows), jnp.int32),
            pltpu.VMEM((top_k, rows), F32),
            pltpu.VMEM((top_k, rows), jnp.int32),
            pltpu.VMEM((d_model // PIECE, group * rows, PIECE), BF16),
            pltpu.VMEM((group, 8, 128), F32),
            pltpu.VMEM((2, cap, group * rows), BF16),
            pltpu.VMEM((group, rows, 12 * cap_local), BF16),
            pltpu.VMEM((2, cap, 1), F32),
            pltpu.VMEM((2, cap, 2 * PIECE), BF16),
            pltpu.VMEM((2, 2, cap, d_ff), F32),
            pltpu.VMEM((2, cap, d_ff), BF16),
            pltpu.VMEM((GU_SLOTS, 2, 2, kw, d_ff), BF16),
            pltpu.VMEM((WD_SLOTS, 2, d_ff, 2 * hu), BF16),
            pltpu.VMEM((N_U, 2, 4, 2 * cap_local, hu), F32),
            pltpu.VMEM((N_U, 4, 2 * cap_local, hu), F32),
            pltpu.VMEM((N_U, 2, rows, hu), F32),
            pltpu.VMEM((N_U, 2, rows, hu), F32),
            pltpu.VMEM((N_U, 2, rows, hu), F32),
            pltpu.VMEM((N_U, rows, hu), F32),
            pltpu.VMEM((N_U, rows, hu), F32),
            pltpu.VMEM((N_U, rows, hu), BF16),
            dma((3,)), dma, dma((GU_SLOTS,)), dma((2,)), dma((WD_SLOTS,)), dma, dma, dma, dma,
            dma, dma((n_k,)), dma, dma, dma, dma((n_k,)),
            dma, dma((N_U,)), dma, dma((N_U, 2)), dma, dma((N_U,)), dma((2,)), dma((2,)),
        ]
        return pl.pallas_call(
            functools.partial(moe_kernel, rows, d_model, d_ff, cap_local),
            out_shape=pltpu.VMEM((rows, d_model), BF16),
            in_specs=[any_spec] * 7,
            out_specs=vmem_spec,
            scratch_shapes=scratch,
            compiler_params=pltpu.CompilerParams(collective_id=0, has_side_effects=True,
                                                 vmem_limit_bytes=66_400_000),
        )(hidden, expert_ids.T, gate_wts.T, slot_pos.T, w_gate, w_up, w_down)

    return jax.shard_map(device_step, mesh=mesh, in_specs=in_specs, out_specs=row_spec, check_vma=False)
```
